32 devices in a mesh: grp: 4 (over x, core), clu: 8 (over z, y).
Axes of the slice: x: 2, y: 2, z: 4, core: 2. Of those that a mesh axis runs over, the one named last changes fastest.
Arguments:
- radiosity: float32 [128, 3, 128], P(('grp', 'clu')), may hold values from 0 to 3
- form_factors: float32 [4096, 128, 128], P(('grp', 'clu')), may hold values from 0.01 to 16
- source_device: int32 [4096, 1], P(('grp', 'clu')), may hold values from 0 to 31; in each aligned block of 128 rows (0 to 127, 128 to 255, ...) at most 8 rows name the same one
- source_slot: int32 [4096], P(('grp', 'clu')), may hold values from 0 to 3
- receiver_slot: int32 [4096], P(('grp', 'clu')), may hold values from 0 to 3
- emission: float32 [128, 3, 128], P(('grp', 'clu')), may hold values from 0.1 to 2
- reflectance: float32 [128, 3, 128], P(('grp', 'clu')), may hold values from 0.3 to 0.9
- patch_area: float32 [128, 128], P(('grp', 'clu')), may hold values from 0.5 to 2
- cluster_group: int32 [128], P(('grp', 'clu')), may hold values from 0 to 15, as said below
- group_coupling: float32 [16, 16], replicated, may hold values from 0 to 1
- ambient: float32 [3], replicated, may hold values from 0.2 to 1
Outputs:
- radiosity_new: float32 [128, 3, 128], P(('grp', 'clu'))
- group_radiosity: float32 [16, 3], replicated
The draws below stay inside these ranges and needn't reach their ends.
Inputs may be any that keep to these rules, and one draw needn't show every extreme that they name: `source_device`: the rows of one device name each source device at most 8 times. `cluster_group`: each group node has exactly 8 clusters.
All inputs are finite; a program needn't handle non-finite values.
Results may differ from the reference program's by a relative error of at most 0.00005.
Values sent between devices are 32-bit elements; how exact they have to be, the bound alone decides.
No kernel may reach another device: no remote copies, remote signals or barrier semaphores. Data moves between devices by JAX's collectives and lax.ppermute only.
A program may use at most 64 MiB of HBM per device.

```python
import math
import jax
import jax.numpy as jnp
import numpy as np
from jax import lax

P_SIZE = 128
CL_DEV = 4
LINKS_DEV = 128
CPG = 8
CLUSTERS = 128
GROUPS = 16
LINKS = 4096
CAP = 8
DEVICES = 32


def draw_cluster_group(key, part):
    return (jax.random.permutation(key, CLUSTERS) // CPG).astype(jnp.int32)


def draw_radiosity(key, part):
    first, second, third = jax.random.split(jax.random.fold_in(key, 11), 3)
    shape = (CLUSTERS, 3, P_SIZE)
    base = jax.random.uniform(first, shape, jnp.float32)
    background = 0.5 * base
    bright = jax.random.bernoulli(second, 1.0 / 32.0, shape)
    level = jax.random.uniform(third, shape, jnp.float32, 2.0, 3.0)
    return jnp.where(bright, level, background).astype(jnp.float32)


def draw_form_factors(key, part):
    first = jax.random.fold_in(jax.random.fold_in(key, 23), 0)
    shape = (LINKS, P_SIZE, P_SIZE)
    low = math.log(0.04)
    high = math.log(16.0)
    values = jnp.exp(jax.random.uniform(first, shape, jnp.float32, low, high))
    return values.astype(jnp.float32)


def place_ends(result, own_key, smallest, top_value):
    dims = result.shape
    index_at = [jax.random.randint(jax.random.fold_in(own_key, axis), (), 0, dims[axis]) for axis in range(len(dims))]
    result = result.at[tuple(index_at)].set(smallest)
    longest = dims.index(max(dims))
    index_at[longest] = (index_at[longest] + 1) % dims[longest]
    return result.at[tuple(index_at)].set(top_value)


def steps_of(rng, shape, cuts, smallest, high):
    level = 1.0
    for position, parts in cuts:
        steps = jax.random.uniform(jax.random.fold_in(jax.random.fold_in(rng, 6), position), (parts,), jnp.float32, smallest / len(cuts), high / len(cuts))
        level = level * jnp.repeat(jnp.exp(steps), shape[position] // parts).reshape((-1,) + (1,) * (len(shape) - 1 - position))
    return level


def shared_out(own_key, own, number, rows, amount, top, limit, slope):
    order = jax.random.permutation(own_key, amount)
    crowded, ordinary = portions_of(amount, rows * top, limit, slope, True), portions_of(amount, rows * top, limit, slope, False)
    places = jnp.arange(amount)

    def named(sizes, offset_by):
        used = int((sizes > 0).sum())
        fixed = max(1, used // 4)
        shifted = fixed + (places - fixed + offset_by * (used - fixed)) % max(1, amount - fixed)
        return jnp.zeros((amount,), jnp.int32).at[order[jnp.where(places < fixed, places, shifted)]].set(jnp.asarray(sizes, jnp.int32))

    sizes = jnp.where(number % 4 == 0, named(crowded, number // 4), named(ordinary, number - number // 4 - 1))
    mixed = jax.random.permutation(jax.random.fold_in(own, 3), amount)
    donor, taker = mixed[0:amount // 2 * 2:2], mixed[1:amount // 2 * 2:2]
    margin = jnp.minimum(sizes[donor] - 1, limit - sizes[taker]) // 2
    margin = jnp.where((donor == order[0]) | (taker == order[0]) | (sizes[taker] == 0), 0, jnp.maximum(margin, 0))
    shifted = jax.random.randint(jax.random.fold_in(own, 4), (amount // 2,), 0, 1 << 20) % (margin + 1)
    sizes = sizes.at[donor].add(-shifted).at[taker].add(shifted)
    labels = jnp.searchsorted(jnp.cumsum(sizes), jnp.arange(rows * top), side="right").astype(jnp.int32)
    grid = labels.reshape(top, rows).T
    grid = grid[jax.random.permutation(jax.random.fold_in(own, 1), rows)]
    offset_by = jax.random.randint(jax.random.fold_in(own, 2), (rows, 1), 0, top)
    return jnp.take_along_axis(grid, (jnp.arange(top)[None, :] + offset_by) % top, axis=1)


def portions_of(number_of, total, most, skew, full):
    portions = [(1 << 20) // math.isqrt(rank ** skew) + 1 for rank in range(1, number_of + 1)]
    largest = most if full else min(most, max(-(-total // number_of), total * portions[0] // sum(portions)))
    least = 1 if total - largest >= number_of - 1 else 0
    counts, rest = [largest] + [least] * (number_of - 1), total - largest - least * (number_of - 1)
    while rest > 0:
        free = [i for i in range(1, number_of) if counts[i] < largest] or [i for i in range(1, number_of) if counts[i] < most]
        whole, remaining = sum([portions[i] for i in free]), rest
        for i in free:
            extra = min(most - counts[i], max(1, remaining * portions[i] // whole), rest)
            counts[i] = counts[i] + extra
            rest = rest - extra
    return np.array(counts)


def setup_inputs(seed: int = 0) -> dict:
    key_list = jax.random.split(jax.random.key(seed), 12)
    radiosity = draw_radiosity(jax.random.fold_in(key_list[11], 71), 0)
    form_factors = draw_form_factors(jax.random.fold_in(key_list[11], 71), 0)
    source_device_keys = jax.random.split(jax.random.fold_in(key_list[2], 1), LINKS // LINKS_DEV)
    source_device_turns = jax.random.permutation(jax.random.fold_in(key_list[2], 3), LINKS // LINKS_DEV)
    source_device = jax.vmap(lambda own, number: shared_out(jax.random.fold_in(key_list[2], 2), own, number, LINKS_DEV, DEVICES, 1, CAP, 2))(source_device_keys, source_device_turns).reshape((LINKS, 1))
    source_slot = place_ends(jax.random.randint(key_list[3], (LINKS,), 0, CL_DEV), jax.random.fold_in(key_list[3], 1), 0, CL_DEV - 1).astype(jnp.int32)
    receiver_slot = place_ends(jax.random.randint(key_list[4], (LINKS,), 0, CL_DEV), jax.random.fold_in(key_list[4], 1), 0, CL_DEV - 1).astype(jnp.int32)
    emission = jnp.clip(jnp.exp(math.log(2.0) - 2.9957323 * jax.random.uniform(key_list[5], (CLUSTERS, 3, P_SIZE), jnp.float32) ** steps_of(key_list[5], (CLUSTERS, 3, P_SIZE), ((0, 32),), -0.2, 0.2)), 0.1, 2.0)
    reflectance = jnp.clip(0.3 + 0.59999996 * jax.random.uniform(key_list[6], (CLUSTERS, 3, P_SIZE), jnp.float32) ** steps_of(key_list[6], (CLUSTERS, 3, P_SIZE), ((0, 32),), -0.2, 0.2), 0.3, 0.9)
    patch_area = jnp.clip(jnp.exp(math.log(2.0) - 1.3862944 * jax.random.uniform(key_list[7], (CLUSTERS, P_SIZE), jnp.float32) ** steps_of(key_list[7], (CLUSTERS, P_SIZE), ((0, 32),), -0.2, 0.2)), 0.5, 2.0)
    cluster_group = draw_cluster_group(jax.random.fold_in(key_list[11], 71), 0)
    group_coupling = jnp.clip(jax.random.uniform(key_list[9], (GROUPS, GROUPS), jnp.float32, 0.0, 1.0), 0.0, 1.0)
    ambient = jnp.clip(jax.random.uniform(key_list[10], (3,), jnp.float32, 0.2, 1.0), 0.2, 1.0)
    return {"radiosity": radiosity, "form_factors": form_factors, "source_device": source_device, "source_slot": source_slot, "receiver_slot": receiver_slot, "emission": emission, "reflectance": reflectance, "patch_area": patch_area, "cluster_group": cluster_group, "group_coupling": group_coupling, "ambient": ambient}


def pull_groups(field, patch_area, cluster_group):
    cluster_sum = jnp.einsum("kci,ki->kc", field, patch_area, precision=lax.Precision.HIGHEST)
    cluster_area = jnp.sum(patch_area, axis=1)
    group_sum = jax.ops.segment_sum(cluster_sum, cluster_group, num_segments=GROUPS)
    group_area = jax.ops.segment_sum(cluster_area, cluster_group, num_segments=GROUPS)
    return group_sum, group_area


def reference(radiosity, form_factors, source_device, source_slot, receiver_slot, emission, reflectance, patch_area, cluster_group, group_coupling, ambient):
    scale = 2.0 * CL_DEV / (P_SIZE * LINKS_DEV)
    rows = jnp.arange(LINKS, dtype=jnp.int32)
    receivers = (rows // LINKS_DEV) * CL_DEV + receiver_slot
    sources = source_device[:, 0] * CL_DEV + source_slot
    fetched = jnp.take(radiosity, sources, axis=0)
    contribution = jnp.einsum("lij,lcj->lci", form_factors, fetched, precision=lax.Precision.HIGHEST) * scale
    irradiance = jax.ops.segment_sum(contribution, receivers, num_segments=CLUSTERS)
    group_sum, group_area = pull_groups(radiosity, patch_area, cluster_group)
    old_group = group_sum / group_area[:, None]
    old_root = jnp.sum(group_sum, axis=0) / jnp.sum(group_area)
    group_irradiance = jnp.dot(group_coupling / GROUPS, old_group, precision=lax.Precision.HIGHEST)
    root_irradiance = ambient * old_root
    coarse = jnp.take(group_irradiance, cluster_group, axis=0) + root_irradiance[None, :]
    total = irradiance + coarse[:, :, None]
    radiosity_new = emission + reflectance * total
    new_sum, new_area = pull_groups(radiosity_new, patch_area, cluster_group)
    return radiosity_new, new_sum / new_area[:, None]
```

```python
import functools

import jax
import jax.numpy as jnp
from jax import lax
from jax.experimental import pallas as pl
from jax.experimental.pallas import tpu as pltpu
from jax.sharding import PartitionSpec as P

LANES = 128
AXES = ("grp", "clu")
VMEM = pl.BlockSpec(memory_space=pltpu.VMEM)
SMEM = pl.BlockSpec(memory_space=pltpu.SMEM)


def rows_for(quantities, groups):
    return -(-quantities // (LANES // groups))


def place(values, cluster_group_ref, groups):
    per_row = LANES // groups
    lane = lax.broadcasted_iota(jnp.int32, (1, LANES), 1)
    rows = [jnp.zeros((1, LANES), jnp.float32) for _ in range(rows_for(len(values), groups))]
    for q, of_clusters in enumerate(values):
        for k, value in enumerate(of_clusters):
            spot = (q % per_row) * groups + cluster_group_ref[k]
            rows[q // per_row] += jnp.where(lane == spot, value, 0.0)
    return rows


def pack_kernel(devices, groups, radiosity_ref, area_ref, cluster_group_ref, out_ref):
    channels, clusters, _ = radiosity_ref.shape
    area = area_ref[...]
    sums = [
        jnp.sum(radiosity_ref[c] * area, axis=1, keepdims=True) for c in range(channels)
    ] + [jnp.sum(area, axis=1, keepdims=True)]
    values = [[s[k : k + 1] for k in range(clusters)] for s in sums]
    info = place(values, cluster_group_ref, groups)
    rows = [radiosity_ref[c, k : k + 1] for c in range(channels) for k in range(clusters)] + info
    block = len(rows)
    for d in range(devices):
        for r, row in enumerate(rows):
            out_ref[d * block + r] = row


def sweep_kernel(
    devices,
    groups,
    scale,
    source_device_ref,
    source_slot_ref,
    receiver_slot_ref,
    cluster_group_ref,
    ambient_ref,
    gathered_ref,
    factors_ref,
    emission_ref,
    reflectance_ref,
    area_ref,
    coupling_ref,
    radiosity_ref,
    share_ref,
    acc_ref,
):
    channels, clusters, width = emission_ref.shape
    count = factors_ref.shape[0]
    blocks = width // 8
    block_rows = gathered_ref.shape[0] // devices
    own_rows = channels * clusters
    per_row = LANES // groups

    acc_ref[...] = jnp.zeros_like(acc_ref)

    totals = []
    for r in range(own_rows, block_rows):
        total = gathered_ref[r]
        for d in range(1, devices):
            total = total + gathered_ref[d * block_rows + r]
        totals.append(total)
    lane = lax.broadcasted_iota(jnp.int32, (1, LANES), 1)
    inside = lane < groups
    parts = []
    for q in range(channels + 1):
        row, shift = totals[q // per_row], (q % per_row) * groups
        part = pltpu.roll(row, LANES - shift, 1) if shift else row
        parts.append(jnp.where(inside, part, 0.0))
    group_area = jnp.where(inside, parts[channels], 1.0)
    all_area = jnp.sum(parts[channels], axis=1, keepdims=True)
    coarse = []
    for c in range(channels):
        old_group = parts[c] / group_area
        root = ambient_ref[c] * (jnp.sum(parts[c], axis=1, keepdims=True) / all_area)
        coarse.append(
            [
                jnp.sum(
                    coupling_ref[pl.ds(cluster_group_ref[k], 1), :] * old_group[:, :groups],
                    axis=1,
                    keepdims=True,
                )
                / groups
                + root
                for k in range(clusters)
            ]
        )

    def link(l, _):
        first = source_device_ref[l] * block_rows + source_slot_ref[l]
        k = receiver_slot_ref[l]
        rows = [
            jnp.broadcast_to(gathered_ref[first + c * clusters], (8, width))
            for c in range(channels)
        ]
        for b in range(blocks):
            f = factors_ref[l, b * 8 : (b + 1) * 8, :]
            for c in range(channels):
                acc_ref[k, c, b] += f * rows[c]
        return 0

    lax.fori_loop(0, count, link, 0, unroll=4)

    patch = lax.broadcasted_iota(jnp.int32, (blocks, 8, width), 0) * 8 + lax.broadcasted_iota(
        jnp.int32, (blocks, 8, width), 1
    )
    diagonal = patch == lax.broadcasted_iota(jnp.int32, (blocks, 8, width), 2)
    sums = [[None] * clusters for _ in range(channels)]
    for k in range(clusters):
        for c in range(channels):
            column = jnp.sum(acc_ref[k, c], axis=2, keepdims=True)
            spread = jnp.sum(jnp.where(diagonal, column, 0.0), axis=0)
            irradiance = jnp.sum(spread, axis=0, keepdims=True) * scale
            new = emission_ref[c, k : k + 1] + reflectance_ref[c, k : k + 1] * (
                irradiance + coarse[c][k]
            )
            radiosity_ref[c, k : k + 1] = new
            sums[c][k] = jnp.sum(new * area_ref[k : k + 1], axis=1, keepdims=True)
    rows = place(sums, cluster_group_ref, groups)
    wide_area = group_area
    for q in range(1, per_row):
        wide_area = jnp.where(lane >= q * groups, pltpu.roll(group_area, q * groups, 1), wide_area)
    for r in range(len(rows)):
        row = rows[r] / wide_area
        for d in range(devices):
            share_ref[d * len(rows) + r] = row


def total_kernel(devices, groups, channels, share_ref, out_ref):
    per_row = LANES // groups
    count = share_ref.shape[0] // devices
    rows = []
    for r in range(count):
        total = share_ref[r]
        for d in range(1, devices):
            total = total + share_ref[d * count + r]
        rows.append(total)
    for c in range(channels):
        row, shift = rows[c // per_row], (c % per_row) * groups
        part = pltpu.roll(row, LANES - shift, 1) if shift else row
        out_ref[c : c + 1, :] = part[:, :groups]


def on_device(
    radiosity,
    form_factors,
    source_device,
    source_slot,
    receiver_slot,
    emission,
    reflectance,
    patch_area,
    cluster_group,
    group_coupling,
    ambient,
):
    clusters, channels, width = radiosity.shape
    count = form_factors.shape[0]
    groups = group_coupling.shape[0]
    devices = lax.axis_size("grp") * lax.axis_size("clu")
    scale = 2.0 * clusters / (width * count)
    block = channels * clusters + rows_for(channels + 1, groups)
    by_channel = functools.partial(jnp.transpose, axes=(1, 0, 2))

    packed = pl.pallas_call(
        functools.partial(pack_kernel, devices, groups),
        out_shape=jax.ShapeDtypeStruct((devices * block, 1, LANES), jnp.float32),
        in_specs=[VMEM, VMEM, SMEM],
        out_specs=VMEM,
        name="pack",
    )(by_channel(radiosity), patch_area, cluster_group)
    gathered = lax.all_to_all(packed, AXES, split_axis=0, concat_axis=0, tiled=True)

    share_rows = rows_for(channels, groups)
    new, share = pl.pallas_call(
        functools.partial(sweep_kernel, devices, groups, scale),
        out_shape=(
            jax.ShapeDtypeStruct((channels, clusters, width), jnp.float32),
            jax.ShapeDtypeStruct((devices * share_rows, 1, LANES), jnp.float32),
        ),
        in_specs=[SMEM] * 5 + [VMEM] * 6,
        out_specs=(VMEM, VMEM),
        scratch_shapes=[pltpu.VMEM((clusters, channels, width // 8, 8, width), jnp.float32)],
        name="sweep",
    )(
        source_device[:, 0],
        source_slot,
        receiver_slot,
        cluster_group,
        ambient,
        gathered,
        form_factors,
        by_channel(emission),
        by_channel(reflectance),
        patch_area,
        group_coupling,
    )
    shares = lax.all_to_all(share, AXES, split_axis=0, concat_axis=0, tiled=True)
    total = pl.pallas_call(
        functools.partial(total_kernel, devices, groups, channels),
        out_shape=jax.ShapeDtypeStruct((channels, groups), jnp.float32),
        in_specs=[VMEM],
        out_specs=VMEM,
        name="total",
    )(shares)
    return by_channel(new), total.T


def solution(mesh):
    split = AXES
    return jax.shard_map(
        on_device,
        mesh=mesh,
        in_specs=(
            P(split, None, None),
            P(split, None, None),
            P(split, None),
            P(split),
            P(split),
            P(split, None, None),
            P(split, None, None),
            P(split, None),
            P(split),
            P(),
            P(),
        ),
        out_specs=(P(split, None, None), P()),
        check_vma=False,
    )
```

```python
import functools

import jax
import jax.numpy as jnp
from jax import lax
from jax.experimental import pallas as pl
from jax.experimental.pallas import tpu as pltpu
from jax.sharding import PartitionSpec as P

LANES = 128
UNROLL = 4
AXES = ("grp", "clu")
VMEM = pl.BlockSpec(memory_space=pltpu.VMEM)
SMEM = pl.BlockSpec(memory_space=pltpu.SMEM)
HBM = pl.BlockSpec(memory_space=pltpu.HBM)
DMA = pltpu.SemaphoreType.DMA


def in_hbm(*arrays):
    return tuple(pltpu.with_memory_space_constraint(a, pltpu.HBM) for a in arrays)


def in_vmem(*arrays):
    return tuple(pltpu.with_memory_space_constraint(a, pltpu.VMEM) for a in arrays)


def rows_for(quantities, groups):
    return -(-quantities // (LANES // groups))


def start_all(pairs, sems):
    copies = [pltpu.make_async_copy(src, dst, sems.at[i]) for i, (src, dst) in enumerate(pairs)]
    for copy in copies:
        copy.start()
    return copies


def pack_kernel(
    devices,
    groups,
    radiosity_hbm,
    area_hbm,
    cluster_group_hbm,
    source_device_hbm,
    source_slot_hbm,
    receiver_slot_hbm,
    ambient_hbm,
    out_ref,
    cluster_group_ref,
    source_device_ref,
    source_slot_ref,
    receiver_slot_ref,
    ambient_ref,
    radiosity_ref,
    area_ref,
    sems,
):
    channels, clusters, _ = radiosity_ref.shape
    per_row = LANES // groups
    copies = start_all(
        (
            (radiosity_hbm, radiosity_ref),
            (area_hbm, area_ref),
            (cluster_group_hbm, cluster_group_ref),
            (source_device_hbm, source_device_ref),
            (source_slot_hbm, source_slot_ref),
            (receiver_slot_hbm, receiver_slot_ref),
            (ambient_hbm, ambient_ref),
        ),
        sems,
    )
    for copy in copies[:3]:
        copy.wait()
    area = area_ref[...]
    sums = [
        jnp.sum(radiosity_ref[c] * area, axis=1, keepdims=True) for c in range(channels)
    ] + [jnp.sum(area, axis=1, keepdims=True)]
    lane = lax.broadcasted_iota(jnp.int32, (1, LANES), 1)
    info = [jnp.zeros((1, LANES), jnp.float32) for _ in range(rows_for(channels + 1, groups))]
    for q in range(channels + 1):
        for k in range(clusters):
            spot = (q % per_row) * groups + cluster_group_ref[k]
            info[q // per_row] += jnp.where(lane == spot, sums[q][k : k + 1], 0.0)
    rows = [radiosity_ref[c, k : k + 1] for c in range(channels) for k in range(clusters)] + info
    block = len(rows)
    for d in range(devices):
        for r, row in enumerate(rows):
            out_ref[d * block + r] = row
    for copy in copies[3:]:
        copy.wait()


def sweep_kernel(
    devices,
    groups,
    scale,
    source_device_ref,
    source_slot_ref,
    receiver_slot_ref,
    cluster_group_ref,
    ambient_ref,
    gathered_ref,
    factors_ref,
    emission_ref,
    reflectance_ref,
    area_ref,
    coupling_ref,
    radiosity_ref,
    share_ref,
    acc_ref,
):
    channels, clusters, width = emission_ref.shape
    count = factors_ref.shape[0]
    blocks = width // 8
    block_rows = gathered_ref.shape[0] // devices
    own_rows = channels * clusters
    per_row = LANES // groups

    acc_ref[...] = jnp.zeros_like(acc_ref)

    totals = []
    for r in range(own_rows, block_rows):
        total = gathered_ref[r]
        for d in range(1, devices):
            total = total + gathered_ref[d * block_rows + r]
        totals.append(total)
    lane = lax.broadcasted_iota(jnp.int32, (1, LANES), 1)
    inside = lane < groups
    parts = []
    for q in range(channels + 1):
        row, shift = totals[q // per_row], (q % per_row) * groups
        part = pltpu.roll(row, LANES - shift, 1) if shift else row
        parts.append(jnp.where(inside, part, 0.0))
    group_area = jnp.where(inside, parts[channels], 1.0)
    all_area = jnp.sum(parts[channels], axis=1, keepdims=True)
    coarse = []
    for c in range(channels):
        old_group = parts[c] / group_area
        root = ambient_ref[c] * (jnp.sum(parts[c], axis=1, keepdims=True) / all_area)
        coarse.append(
            [
                jnp.sum(
                    coupling_ref[pl.ds(cluster_group_ref[k], 1), :] * old_group[:, :groups],
                    axis=1,
                    keepdims=True,
                )
                / groups
                + root
                for k in range(clusters)
            ]
        )

    def link(l, _):
        first = source_device_ref[l] * block_rows + source_slot_ref[l]
        k = receiver_slot_ref[l]
        rows = [
            jnp.broadcast_to(gathered_ref[first + c * clusters], (8, width))
            for c in range(channels)
        ]
        for b in range(blocks):
            f = factors_ref[l, b * 8 : (b + 1) * 8, :]
            for c in range(channels):
                acc_ref[k, c, b] += f * rows[c]
        return 0

    lax.fori_loop(0, count, link, 0, unroll=UNROLL)

    patch = lax.broadcasted_iota(jnp.int32, (blocks, 8, width), 0) * 8 + lax.broadcasted_iota(
        jnp.int32, (blocks, 8, width), 1
    )
    diagonal = patch == lax.broadcasted_iota(jnp.int32, (blocks, 8, width), 2)
    sums = [[None] * clusters for _ in range(channels)]
    for k in range(clusters):
        for c in range(channels):
            column = jnp.sum(acc_ref[k, c], axis=2, keepdims=True)
            spread = jnp.sum(jnp.where(diagonal, column, 0.0), axis=0)
            irradiance = jnp.sum(spread, axis=0, keepdims=True) * scale
            new = emission_ref[c, k : k + 1] + reflectance_ref[c, k : k + 1] * (
                irradiance + coarse[c][k]
            )
            radiosity_ref[c, k : k + 1] = new
            sums[c][k] = jnp.sum(new * area_ref[k : k + 1], axis=1, keepdims=True)
    shares = [jnp.zeros((1, LANES), jnp.float32) for _ in range(rows_for(channels, groups))]
    for c in range(channels):
        for k in range(clusters):
            spot = (c % per_row) * groups + cluster_group_ref[k]
            shares[c // per_row] += jnp.where(lane == spot, sums[c][k], 0.0)
    wide_area = group_area
    for q in range(1, per_row):
        wide_area = jnp.where(lane >= q * groups, pltpu.roll(group_area, q * groups, 1), wide_area)
    for r in range(len(shares)):
        row = shares[r] / wide_area
        for d in range(devices):
            share_ref[d * len(shares) + r] = row


def total_kernel(devices, groups, share_ref, new_ref, new_hbm, total_hbm, total_ref, sems):
    channels = new_ref.shape[0]
    per_row = LANES // groups
    count = share_ref.shape[0] // devices
    new_copy = pltpu.make_async_copy(new_ref, new_hbm, sems.at[0])
    new_copy.start()
    rows = []
    for r in range(count):
        total = share_ref[r]
        for d in range(1, devices):
            total = total + share_ref[d * count + r]
        rows.append(total)
    for c in range(channels):
        row, shift = rows[c // per_row], (c % per_row) * groups
        part = pltpu.roll(row, LANES - shift, 1) if shift else row
        total_ref[c : c + 1, :] = part[:, :groups]
    total_copy = pltpu.make_async_copy(total_ref, total_hbm, sems.at[1])
    total_copy.start()
    new_copy.wait()
    total_copy.wait()


def on_device(
    radiosity,
    form_factors,
    source_device,
    source_slot,
    receiver_slot,
    emission,
    reflectance,
    patch_area,
    cluster_group,
    group_coupling,
    ambient,
):
    clusters, channels, width = radiosity.shape
    count = form_factors.shape[0]
    groups = group_coupling.shape[0]
    devices = lax.axis_size("grp") * lax.axis_size("clu")
    scale = 2.0 * clusters / (width * count)
    block = channels * clusters + rows_for(channels + 1, groups)
    by_channel = functools.partial(jnp.transpose, axes=(1, 0, 2))
    f32, i32 = jnp.float32, jnp.int32
    own = pltpu.VMEM((channels, clusters, width), f32)

    packed, cluster_group, source_device, source_slot, receiver_slot, ambient = pl.pallas_call(
        functools.partial(pack_kernel, devices, groups),
        out_shape=(
            pltpu.VMEM((devices * block, 1, LANES), f32),
            pltpu.SMEM((clusters,), i32),
            pltpu.SMEM((count,), i32),
            pltpu.SMEM((count,), i32),
            pltpu.SMEM((count,), i32),
            pltpu.SMEM((channels,), f32),
        ),
        in_specs=[HBM] * 7,
        out_specs=(VMEM,) + (SMEM,) * 5,
        scratch_shapes=[
            pltpu.VMEM((channels, clusters, width), f32),
            pltpu.VMEM((clusters, width), f32),
            DMA((7,)),
        ],
        compiler_params=pltpu.CompilerParams(vmem_limit_bytes=4 << 20),
        cost_estimate=pl.CostEstimate(flops=10**10, transcendentals=0, bytes_accessed=10**8),
        name="pack",
    )(
        *in_hbm(
            by_channel(radiosity),
            patch_area,
            cluster_group,
            source_device[:, 0],
            source_slot,
            receiver_slot,
            ambient,
        )
    )
    gathered = lax.all_to_all(packed, AXES, split_axis=0, concat_axis=0, tiled=True)

    share_rows = rows_for(channels, groups)
    new, share = pl.pallas_call(
        functools.partial(sweep_kernel, devices, groups, scale),
        out_shape=(own, pltpu.VMEM((devices * share_rows, 1, LANES), f32)),
        in_specs=[SMEM] * 5 + [VMEM] * 6,
        out_specs=(VMEM, VMEM),
        scratch_shapes=[pltpu.VMEM((clusters, channels, width // 8, 8, width), f32)],
        compiler_params=pltpu.CompilerParams(vmem_limit_bytes=16 << 20),
        name="sweep",
    )(
        source_device,
        source_slot,
        receiver_slot,
        cluster_group,
        ambient,
        *in_vmem(
            gathered,
            form_factors,
            by_channel(emission),
            by_channel(reflectance),
            patch_area,
            group_coupling,
        ),
    )
    shares = lax.all_to_all(share, AXES, split_axis=0, concat_axis=0, tiled=True)
    new, total = pl.pallas_call(
        functools.partial(total_kernel, devices, groups),
        out_shape=(
            pltpu.HBM((channels, clusters, width), f32),
            pltpu.HBM((channels, groups), f32),
        ),
        in_specs=[VMEM, VMEM],
        out_specs=(HBM, HBM),
        scratch_shapes=[pltpu.VMEM((channels, groups), f32), DMA((2,))],
        compiler_params=pltpu.CompilerParams(vmem_limit_bytes=4 << 20),
        name="total",
    )(*in_vmem(shares, new))
    return by_channel(new), total.T


def solution(mesh):
    split = AXES
    return jax.shard_map(
        on_device,
        mesh=mesh,
        in_specs=(
            P(split, None, None),
            P(split, None, None),
            P(split, None),
            P(split),
            P(split),
            P(split, None, None),
            P(split, None, None),
            P(split, None),
            P(split),
            P(),
            P(),
        ),
        out_specs=(P(split, None, None), P()),
        check_vma=False,
    )
```

```python
import functools

import jax
import jax.numpy as jnp
from jax import lax
from jax.experimental import pallas as pl
from jax.experimental.pallas import tpu as pltpu
from jax.sharding import PartitionSpec as P

LANES = 128
UNROLL = 4
STEP = 8
AXES = ("grp", "clu")
VMEM = pl.BlockSpec(memory_space=pltpu.VMEM)
SMEM = pl.BlockSpec(memory_space=pltpu.SMEM)
HBM = pl.BlockSpec(memory_space=pltpu.HBM)
DMA = pltpu.SemaphoreType.DMA


def in_hbm(*arrays):
    return tuple(pltpu.with_memory_space_constraint(a, pltpu.HBM) for a in arrays)


def in_vmem(*arrays):
    return tuple(pltpu.with_memory_space_constraint(a, pltpu.VMEM) for a in arrays)


def rows_for(quantities, groups):
    return -(-quantities // (LANES // groups))


def start_all(pairs, sems):
    copies = [pltpu.make_async_copy(src, dst, sems.at[i]) for i, (src, dst) in enumerate(pairs)]
    for copy in copies:
        copy.start()
    return copies


def pack_kernel(
    devices,
    pair_stride,
    groups,
    radiosity_hbm,
    area_hbm,
    cluster_group_hbm,
    source_device_hbm,
    source_slot_hbm,
    receiver_slot_hbm,
    ambient_hbm,
    out_ref,
    cluster_group_ref,
    source_device_ref,
    source_slot_ref,
    receiver_slot_ref,
    ambient_ref,
    radiosity_ref,
    area_ref,
    sems,
):
    channels, clusters, _ = radiosity_ref.shape
    per_row = LANES // groups
    copies = start_all(
        (
            (radiosity_hbm, radiosity_ref),
            (area_hbm, area_ref),
            (cluster_group_hbm, cluster_group_ref),
            (source_device_hbm, source_device_ref),
            (source_slot_hbm, source_slot_ref),
            (receiver_slot_hbm, receiver_slot_ref),
            (ambient_hbm, ambient_ref),
        ),
        sems,
    )
    for copy in copies[:3]:
        copy.wait()
    area = area_ref[...]
    sums = [
        jnp.sum(radiosity_ref[c] * area, axis=1, keepdims=True) for c in range(channels)
    ] + [jnp.sum(area, axis=1, keepdims=True)]
    lane = lax.broadcasted_iota(jnp.int32, (1, LANES), 1)
    info = [jnp.zeros((1, LANES), jnp.float32) for _ in range(rows_for(channels + 1, groups))]
    for q in range(channels + 1):
        for k in range(clusters):
            spot = (q % per_row) * groups + cluster_group_ref[k]
            info[q // per_row] += jnp.where(lane == spot, sums[q][k : k + 1], 0.0)
    half = clusters // 2
    halves = [
        [(0, k) for k in range(clusters)] + [(1, k) for k in range(half)],
        [(2, k) for k in range(clusters)] + [(1, k) for k in range(half, clusters)],
    ]
    block = len(halves[0]) + len(info)
    for d in range(devices):
        rows = [radiosity_ref[c, k : k + 1] for c, k in halves[d // pair_stride % 2]] + info
        for r, row in enumerate(rows):
            out_ref[d * block + r] = row
    for copy in copies[3:]:
        copy.wait()


def column_sums(acc, diagonal):
    column = jnp.sum(acc, axis=2, keepdims=True)
    spread = jnp.sum(jnp.where(diagonal, column, 0.0), axis=0)
    return jnp.sum(spread, axis=0, keepdims=True)


def diagonal_mask(width):
    shape = (width // 8, 8, width)
    patch = lax.broadcasted_iota(jnp.int32, shape, 0) * 8 + lax.broadcasted_iota(jnp.int32, shape, 1)
    return patch == lax.broadcasted_iota(jnp.int32, shape, 2)


def first_kernel(
    devices,
    groups,
    source_device_ref,
    source_slot_ref,
    receiver_slot_ref,
    cluster_group_ref,
    ambient_ref,
    own_ref,
    factors_ref,
    coupling_ref,
    plan_ref,
    rows_ref,
    acc_ref,
):
    count, width, _ = factors_ref.shape
    clusters, blocks = acc_ref.shape[:2]
    channels = ambient_ref.shape[0]
    capacity = count + STEP
    table = clusters * capacity
    half = clusters // 2
    block_rows = own_ref.shape[0] // devices
    own_rows = clusters + half
    per_row = LANES // groups
    core = lax.rem(lax.axis_index("grp"), 2)

    acc_ref[...] = jnp.zeros_like(acc_ref)

    totals = []
    for r in range(own_rows, block_rows):
        total = own_ref[r]
        for d in range(1, devices):
            total = total + own_ref[d * block_rows + r]
        totals.append(total)
    lane = lax.broadcasted_iota(jnp.int32, (1, LANES), 1)
    inside = lane < groups
    parts = []
    for q in range(channels + 1):
        row, shift = totals[q // per_row], (q % per_row) * groups
        part = pltpu.roll(row, LANES - shift, 1) if shift else row
        parts.append(jnp.where(inside, part, 0.0))
    group_area = jnp.where(inside, parts[channels], 1.0)
    all_area = jnp.sum(parts[channels], axis=1, keepdims=True)
    for c in range(channels):
        old_group = parts[c] / group_area
        root = ambient_ref[c] * (jnp.sum(parts[c], axis=1, keepdims=True) / all_area)
        for k in range(clusters):
            coupling = coupling_ref[pl.ds(cluster_group_ref[k], 1), :]
            coarse = (
                jnp.sum(coupling * old_group[:, :groups], axis=1, keepdims=True) / groups + root
            )
            rows_ref[clusters + c * clusters + k] = jnp.broadcast_to(coarse, (1, LANES))
    wide_area = group_area
    for q in range(1, per_row):
        wide_area = jnp.where(lane >= q * groups, pltpu.roll(group_area, q * groups, 1), wide_area)
    rows_ref[clusters + channels * clusters] = wide_area

    def link(l, filled):
        k = receiver_slot_ref[l]
        slot = source_slot_ref[l]
        base = source_device_ref[l] * block_rows
        spot = k * capacity + (lax.shift_right_arithmetic(filled, k * 8) & 255)
        upper = (slot >= half).astype(jnp.int32)
        mine = (upper == core).astype(jnp.int32)
        plan_ref[spot] = l
        plan_ref[table + spot] = base + slot
        plan_ref[2 * table + spot] = (base + clusters + slot - upper * half) * 2 + mine
        row = jnp.broadcast_to(own_ref[base + slot], (8, width))
        for b in range(blocks):
            acc_ref[k, b] += factors_ref[l, b * 8 : (b + 1) * 8, :] * row
        return filled + lax.shift_left(jnp.int32(1), k * 8)

    filled = lax.fori_loop(0, count, link, jnp.int32(0), unroll=UNROLL)
    for k in range(clusters):
        length = lax.shift_right_arithmetic(filled, jnp.int32(k * 8)) & 255
        plan_ref[3 * table + k] = length
        for i in range(STEP - 1):
            for part in range(3):
                plan_ref[part * table + k * capacity + length + i] = 0

    diagonal = diagonal_mask(width)
    for k in range(clusters):
        rows_ref[k] = column_sums(acc_ref[k], diagonal)


def second_kernel(
    devices,
    groups,
    scale,
    plan_ref,
    cluster_group_ref,
    own_ref,
    other_ref,
    factors_ref,
    rows_ref,
    emission_ref,
    reflectance_ref,
    area_ref,
    radiosity_ref,
    share_ref,
    acc_ref,
):
    channels, clusters, width = emission_ref.shape
    count = factors_ref.shape[0]
    capacity = count + STEP
    table = clusters * capacity
    blocks = width // 8
    per_row = LANES // groups
    core = lax.rem(lax.axis_index("grp"), 2)

    acc_ref[...] = jnp.zeros_like(acc_ref)
    for k in range(clusters):
        length = plan_ref[3 * table + k]

        def step(j, _, k=k, length=length):
            links, pairs = [], []
            for u in range(STEP):
                spot = k * capacity + j * STEP + u
                links.append(plan_ref[spot])
                outer = other_ref[plan_ref[table + spot]]
                code = plan_ref[2 * table + spot]
                middle = lax.shift_right_logical(code, jnp.int32(1))
                inner = jnp.where((code & 1) == 1, own_ref[middle], other_ref[middle])
                valid = j * STEP + u < length
                pairs.append(
                    [
                        jnp.broadcast_to(jnp.where(valid, row, 0.0), (8, width))
                        for row in (inner, outer)
                    ]
                )
            for b in range(blocks):
                acc = [acc_ref[k, r, b] for r in range(2)]
                for u in range(STEP):
                    f = factors_ref[links[u], b * 8 : (b + 1) * 8, :]
                    for r in range(2):
                        acc[r] += f * pairs[u][r]
                for r in range(2):
                    acc_ref[k, r, b] = acc[r]
            return 0

        lax.fori_loop(0, lax.div(length + STEP - 1, STEP), step, 0)

    diagonal = diagonal_mask(width)
    lane = lax.broadcasted_iota(jnp.int32, (1, LANES), 1)
    shares = [jnp.zeros((1, LANES), jnp.float32) for _ in range(rows_for(channels, groups))]
    for k in range(clusters):
        mine = rows_ref[k]
        middle = column_sums(acc_ref[k, 0], diagonal)
        others = column_sums(acc_ref[k, 1], diagonal)
        by_channel = (
            jnp.where(core == 0, mine, others),
            middle,
            jnp.where(core == 0, others, mine),
        )
        for c in range(channels):
            coarse = rows_ref[clusters + c * clusters + k]
            new = emission_ref[c, k : k + 1] + reflectance_ref[c, k : k + 1] * (
                by_channel[c] * scale + coarse
            )
            radiosity_ref[c, k : k + 1] = new
            pulled = jnp.sum(new * area_ref[k : k + 1], axis=1, keepdims=True)
            spot = (c % per_row) * groups + cluster_group_ref[k]
            shares[c // per_row] += jnp.where(lane == spot, pulled, 0.0)
    for r in range(len(shares)):
        row = shares[r] / rows_ref[clusters + channels * clusters]
        for d in range(devices):
            share_ref[d * len(shares) + r] = row


def total_kernel(devices, groups, share_ref, new_ref, new_hbm, total_hbm, total_ref, sems):
    channels = new_ref.shape[0]
    per_row = LANES // groups
    count = share_ref.shape[0] // devices
    new_copy = pltpu.make_async_copy(new_ref, new_hbm, sems.at[0])
    new_copy.start()
    rows = []
    for r in range(count):
        total = share_ref[r]
        for d in range(1, devices):
            total = total + share_ref[d * count + r]
        rows.append(total)
    for c in range(channels):
        row, shift = rows[c // per_row], (c % per_row) * groups
        part = pltpu.roll(row, LANES - shift, 1) if shift else row
        total_ref[c : c + 1, :] = part[:, :groups]
    total_copy = pltpu.make_async_copy(total_ref, total_hbm, sems.at[1])
    total_copy.start()
    new_copy.wait()
    total_copy.wait()


def on_device(
    radiosity,
    form_factors,
    source_device,
    source_slot,
    receiver_slot,
    emission,
    reflectance,
    patch_area,
    cluster_group,
    group_coupling,
    ambient,
):
    clusters, channels, width = radiosity.shape
    count = form_factors.shape[0]
    groups = group_coupling.shape[0]
    devices = lax.axis_size("grp") * lax.axis_size("clu")
    scale = 2.0 * clusters / (width * count)
    pair_stride = lax.axis_size("clu")
    block = clusters + clusters // 2 + rows_for(channels + 1, groups)
    plan_size = 3 * clusters * (count + STEP) + clusters
    by_channel = functools.partial(jnp.transpose, axes=(1, 0, 2))
    f32, i32 = jnp.float32, jnp.int32
    own = pltpu.VMEM((channels, clusters, width), f32)

    packed, cluster_group, source_device, source_slot, receiver_slot, ambient = pl.pallas_call(
        functools.partial(pack_kernel, devices, pair_stride, groups),
        out_shape=(
            pltpu.VMEM((devices * block, 1, LANES), f32),
            pltpu.SMEM((clusters,), i32),
            pltpu.SMEM((count,), i32),
            pltpu.SMEM((count,), i32),
            pltpu.SMEM((count,), i32),
            pltpu.SMEM((channels,), f32),
        ),
        in_specs=[HBM] * 7,
        out_specs=(VMEM,) + (SMEM,) * 5,
        scratch_shapes=[
            pltpu.VMEM((channels, clusters, width), f32),
            pltpu.VMEM((clusters, width), f32),
            DMA((7,)),
        ],
        compiler_params=pltpu.CompilerParams(vmem_limit_bytes=4 << 20),
        cost_estimate=pl.CostEstimate(flops=10**10, transcendentals=0, bytes_accessed=10**8),
        name="pack",
    )(
        *in_hbm(
            by_channel(radiosity),
            patch_area,
            cluster_group,
            source_device[:, 0],
            source_slot,
            receiver_slot,
            ambient,
        )
    )
    own_half = lax.all_to_all(packed, AXES, split_axis=0, concat_axis=0, tiled=True)
    other_half = lax.ppermute(
        own_half, "grp", [(i, i ^ 1) for i in range(lax.axis_size("grp"))]
    )

    plan, rows = pl.pallas_call(
        functools.partial(first_kernel, devices, groups),
        out_shape=(
            pltpu.SMEM((plan_size,), i32),
            pltpu.VMEM((clusters + channels * clusters + 1, 1, LANES), f32),
        ),
        in_specs=[SMEM] * 5 + [VMEM] * 3,
        out_specs=(SMEM, VMEM),
        scratch_shapes=[pltpu.VMEM((clusters, width // 8, 8, width), f32)],
        compiler_params=pltpu.CompilerParams(vmem_limit_bytes=16 << 20),
        cost_estimate=pl.CostEstimate(flops=10**8, transcendentals=0, bytes_accessed=10**7),
        name="first",
    )(
        source_device,
        source_slot,
        receiver_slot,
        cluster_group,
        ambient,
        *in_vmem(own_half, form_factors, group_coupling),
    )
    share_rows = rows_for(channels, groups)
    new, share = pl.pallas_call(
        functools.partial(second_kernel, devices, groups, scale),
        out_shape=(own, pltpu.VMEM((devices * share_rows, 1, LANES), f32)),
        in_specs=[SMEM] * 2 + [VMEM] * 7,
        out_specs=(VMEM, VMEM),
        scratch_shapes=[pltpu.VMEM((clusters, 2, width // 8, 8, width), f32)],
        compiler_params=pltpu.CompilerParams(vmem_limit_bytes=16 << 20),
        name="second",
    )(
        plan,
        cluster_group,
        *in_vmem(
            own_half,
            other_half,
            form_factors,
            rows,
            by_channel(emission),
            by_channel(reflectance),
            patch_area,
        ),
    )
    shares = lax.all_to_all(share, AXES, split_axis=0, concat_axis=0, tiled=True)
    new, total = pl.pallas_call(
        functools.partial(total_kernel, devices, groups),
        out_shape=(
            pltpu.HBM((channels, clusters, width), f32),
            pltpu.HBM((channels, groups), f32),
        ),
        in_specs=[VMEM, VMEM],
        out_specs=(HBM, HBM),
        scratch_shapes=[pltpu.VMEM((channels, groups), f32), DMA((2,))],
        compiler_params=pltpu.CompilerParams(vmem_limit_bytes=4 << 20),
        name="total",
    )(*in_vmem(shares, new))
    return by_channel(new), total.T


def solution(mesh):
    split = AXES
    return jax.shard_map(
        on_device,
        mesh=mesh,
        in_specs=(
            P(split, None, None),
            P(split, None, None),
            P(split, None),
            P(split),
            P(split),
            P(split, None, None),
            P(split, None, None),
            P(split, None),
            P(split),
            P(),
            P(),
        ),
        out_specs=(P(split, None, None), P()),
        check_vma=False,
    )
```

```python
import functools

import jax
import jax.numpy as jnp
from jax import lax
from jax.experimental import pallas as pl
from jax.experimental.pallas import tpu as pltpu
from jax.sharding import PartitionSpec as P

LANES = 128
UNROLL = 8
BANKS = 2
AXES = ("grp", "clu")
VMEM = pl.BlockSpec(memory_space=pltpu.VMEM)
SMEM = pl.BlockSpec(memory_space=pltpu.SMEM)
HBM = pl.BlockSpec(memory_space=pltpu.HBM)
DMA = pltpu.SemaphoreType.DMA


def in_hbm(*arrays):
    return tuple(pltpu.with_memory_space_constraint(a, pltpu.HBM) for a in arrays)


def in_vmem(*arrays):
    return tuple(pltpu.with_memory_space_constraint(a, pltpu.VMEM) for a in arrays)


def rows_for(quantities, groups):
    return -(-quantities // (LANES // groups))


def start_all(pairs, sems):
    copies = [pltpu.make_async_copy(src, dst, sems.at[i]) for i, (src, dst) in enumerate(pairs)]
    for copy in copies:
        copy.start()
    return copies


def pack_kernel(
    devices,
    pair_stride,
    groups,
    radiosity_hbm,
    area_hbm,
    cluster_group_hbm,
    source_device_hbm,
    source_slot_hbm,
    receiver_slot_hbm,
    ambient_hbm,
    out_ref,
    cluster_group_ref,
    source_device_ref,
    source_slot_ref,
    receiver_slot_ref,
    ambient_ref,
    radiosity_ref,
    area_ref,
    sems,
):
    channels, clusters, _ = radiosity_ref.shape
    per_row = LANES // groups
    copies = start_all(
        (
            (radiosity_hbm, radiosity_ref),
            (area_hbm, area_ref),
            (cluster_group_hbm, cluster_group_ref),
            (source_device_hbm, source_device_ref),
            (source_slot_hbm, source_slot_ref),
            (receiver_slot_hbm, receiver_slot_ref),
            (ambient_hbm, ambient_ref),
        ),
        sems,
    )
    for copy in copies[:3]:
        copy.wait()
    area = area_ref[...]
    sums = [
        jnp.sum(radiosity_ref[c] * area, axis=1, keepdims=True) for c in range(channels)
    ] + [jnp.sum(area, axis=1, keepdims=True)]
    lane = lax.broadcasted_iota(jnp.int32, (1, LANES), 1)
    info = [jnp.zeros((1, LANES), jnp.float32) for _ in range(rows_for(channels + 1, groups))]
    for q in range(channels + 1):
        for k in range(clusters):
            spot = (q % per_row) * groups + cluster_group_ref[k]
            info[q // per_row] += jnp.where(lane == spot, sums[q][k : k + 1], 0.0)
    half = clusters // 2
    halves = [
        [(0, k) for k in range(clusters)] + [(1, k) for k in range(half)],
        [(2, k) for k in range(clusters)] + [(1, k) for k in range(half, clusters)],
    ]
    block = len(halves[0]) + len(info)
    for d in range(devices):
        rows = [radiosity_ref[c, k : k + 1] for c, k in halves[d // pair_stride % 2]] + info
        for r, row in enumerate(rows):
            out_ref[d * block + r] = row
    for copy in copies[3:]:
        copy.wait()


def column_sums(acc, diagonal):
    column = jnp.sum(acc, axis=2, keepdims=True)
    spread = jnp.sum(jnp.where(diagonal, column, 0.0), axis=0)
    return jnp.sum(spread, axis=0, keepdims=True)


def diagonal_mask(width):
    shape = (width // 8, 8, width)
    patch = lax.broadcasted_iota(jnp.int32, shape, 0) * 8 + lax.broadcasted_iota(jnp.int32, shape, 1)
    return patch == lax.broadcasted_iota(jnp.int32, shape, 2)


def first_kernel(
    devices,
    groups,
    source_device_ref,
    source_slot_ref,
    receiver_slot_ref,
    cluster_group_ref,
    ambient_ref,
    own_ref,
    factors_ref,
    coupling_ref,
    rows_ref,
    *acc_refs,
):
    count, width, _ = factors_ref.shape
    clusters, blocks = acc_refs[0].shape[:2]
    channels = ambient_ref.shape[0]
    half = clusters // 2
    block_rows = own_ref.shape[0] // devices
    own_rows = clusters + half
    per_row = LANES // groups

    for acc_ref in acc_refs:
        acc_ref[...] = jnp.zeros_like(acc_ref)

    def step(group, carried):
        for u in range(UNROLL):
            l = group * UNROLL + u
            k = receiver_slot_ref[l]
            place = source_device_ref[l] * block_rows + source_slot_ref[l]
            row = jnp.broadcast_to(own_ref[place], (8, width))
            acc_ref = acc_refs[u % len(acc_refs)]
            for b in range(blocks):
                acc_ref[k, b] += factors_ref[l, b * 8 : (b + 1) * 8, :] * row
        return carried

    lax.fori_loop(0, count // UNROLL, step, 0)

    totals = []
    for r in range(own_rows, block_rows):
        total = own_ref[r]
        for d in range(1, devices):
            total = total + own_ref[d * block_rows + r]
        totals.append(total)
    lane = lax.broadcasted_iota(jnp.int32, (1, LANES), 1)
    inside = lane < groups
    parts = []
    for q in range(channels + 1):
        row, shift = totals[q // per_row], (q % per_row) * groups
        part = pltpu.roll(row, LANES - shift, 1) if shift else row
        parts.append(jnp.where(inside, part, 0.0))
    group_area = jnp.where(inside, parts[channels], 1.0)
    all_area = jnp.sum(parts[channels], axis=1, keepdims=True)
    for c in range(channels):
        old_group = parts[c] / group_area
        root = ambient_ref[c] * (jnp.sum(parts[c], axis=1, keepdims=True) / all_area)
        for k in range(clusters):
            coupling = coupling_ref[pl.ds(cluster_group_ref[k], 1), :]
            coarse = (
                jnp.sum(coupling * old_group[:, :groups], axis=1, keepdims=True) / groups + root
            )
            rows_ref[clusters + c * clusters + k] = jnp.broadcast_to(coarse, (1, LANES))
    wide_area = group_area
    for q in range(1, per_row):
        wide_area = jnp.where(lane >= q * groups, pltpu.roll(group_area, q * groups, 1), wide_area)
    rows_ref[clusters + channels * clusters] = wide_area

    diagonal = diagonal_mask(width)
    for k in range(clusters):
        rows_ref[k] = column_sums(sum(acc_ref[k] for acc_ref in acc_refs), diagonal)


def second_kernel(
    devices,
    groups,
    scale,
    source_device_ref,
    source_slot_ref,
    receiver_slot_ref,
    cluster_group_ref,
    own_ref,
    other_ref,
    factors_ref,
    rows_ref,
    emission_ref,
    reflectance_ref,
    area_ref,
    radiosity_ref,
    share_ref,
    *acc_refs,
):
    channels, clusters, width = emission_ref.shape
    count = factors_ref.shape[0]
    half = clusters // 2
    blocks = width // 8
    block_rows = own_ref.shape[0] // devices
    per_row = LANES // groups
    core = lax.rem(lax.axis_index("grp"), 2)

    for acc_ref in acc_refs:
        acc_ref[...] = jnp.zeros_like(acc_ref)

    def step(group, carried):
        for u in range(UNROLL):
            l = group * UNROLL + u
            k, slot = receiver_slot_ref[l], source_slot_ref[l]
            base = source_device_ref[l] * block_rows
            upper = (slot >= half).astype(jnp.int32)
            inner = base + slot - half * upper + clusters
            middle = jnp.where(
                upper == core,
                jnp.broadcast_to(own_ref[inner], (8, width)),
                jnp.broadcast_to(other_ref[inner], (8, width)),
            )
            rows = (middle, jnp.broadcast_to(other_ref[base + slot], (8, width)))
            acc_ref = acc_refs[u % len(acc_refs)]
            for b in range(blocks):
                f = factors_ref[l, b * 8 : (b + 1) * 8, :]
                for r in range(2):
                    acc_ref[k, r, b] += f * rows[r]
        return carried

    lax.fori_loop(0, count // UNROLL, step, 0)

    diagonal = diagonal_mask(width)
    lane = lax.broadcasted_iota(jnp.int32, (1, LANES), 1)
    shares = [jnp.zeros((1, LANES), jnp.float32) for _ in range(rows_for(channels, groups))]
    for k in range(clusters):
        mine = rows_ref[k]
        middle = column_sums(sum(acc_ref[k, 0] for acc_ref in acc_refs), diagonal)
        others = column_sums(sum(acc_ref[k, 1] for acc_ref in acc_refs), diagonal)
        by_channel = (
            jnp.where(core == 0, mine, others),
            middle,
            jnp.where(core == 0, others, mine),
        )
        for c in range(channels):
            coarse = rows_ref[clusters + c * clusters + k]
            new = emission_ref[c, k : k + 1] + reflectance_ref[c, k : k + 1] * (
                by_channel[c] * scale + coarse
            )
            radiosity_ref[c, k : k + 1] = new
            pulled = jnp.sum(new * area_ref[k : k + 1], axis=1, keepdims=True)
            spot = (c % per_row) * groups + cluster_group_ref[k]
            shares[c // per_row] += jnp.where(lane == spot, pulled, 0.0)
    for r in range(len(shares)):
        row = shares[r] / rows_ref[clusters + channels * clusters]
        for d in range(devices):
            share_ref[d * len(shares) + r] = row


def total_kernel(devices, groups, share_ref, new_ref, new_hbm, total_hbm, total_ref, sems):
    channels = new_ref.shape[0]
    per_row = LANES // groups
    count = share_ref.shape[0] // devices
    new_copy = pltpu.make_async_copy(new_ref, new_hbm, sems.at[0])
    new_copy.start()
    rows = []
    for r in range(count):
        total = share_ref[r]
        for d in range(1, devices):
            total = total + share_ref[d * count + r]
        rows.append(total)
    for c in range(channels):
        row, shift = rows[c // per_row], (c % per_row) * groups
        part = pltpu.roll(row, LANES - shift, 1) if shift else row
        total_ref[c : c + 1, :] = part[:, :groups]
    total_copy = pltpu.make_async_copy(total_ref, total_hbm, sems.at[1])
    total_copy.start()
    new_copy.wait()
    total_copy.wait()


def on_device(
    radiosity,
    form_factors,
    source_device,
    source_slot,
    receiver_slot,
    emission,
    reflectance,
    patch_area,
    cluster_group,
    group_coupling,
    ambient,
):
    clusters, channels, width = radiosity.shape
    count = form_factors.shape[0]
    groups = group_coupling.shape[0]
    devices = lax.axis_size("grp") * lax.axis_size("clu")
    scale = 2.0 * clusters / (width * count)
    pair_stride = lax.axis_size("clu")
    block = clusters + clusters // 2 + rows_for(channels + 1, groups)
    by_channel = functools.partial(jnp.transpose, axes=(1, 0, 2))
    f32, i32 = jnp.float32, jnp.int32
    own = pltpu.VMEM((channels, clusters, width), f32)

    packed, cluster_group, source_device, source_slot, receiver_slot, ambient = pl.pallas_call(
        functools.partial(pack_kernel, devices, pair_stride, groups),
        out_shape=(
            pltpu.VMEM((devices * block, 1, LANES), f32),
            pltpu.SMEM((clusters,), i32),
            pltpu.SMEM((count,), i32),
            pltpu.SMEM((count,), i32),
            pltpu.SMEM((count,), i32),
            pltpu.SMEM((channels,), f32),
        ),
        in_specs=[HBM] * 7,
        out_specs=(VMEM,) + (SMEM,) * 5,
        scratch_shapes=[
            pltpu.VMEM((channels, clusters, width), f32),
            pltpu.VMEM((clusters, width), f32),
            DMA((7,)),
        ],
        compiler_params=pltpu.CompilerParams(vmem_limit_bytes=4 << 20),
        cost_estimate=pl.CostEstimate(flops=10**10, transcendentals=0, bytes_accessed=10**8),
        name="pack",
    )(
        *in_hbm(
            by_channel(radiosity),
            patch_area,
            cluster_group,
            source_device[:, 0],
            source_slot,
            receiver_slot,
            ambient,
        )
    )
    own_half = lax.all_to_all(packed, AXES, split_axis=0, concat_axis=0, tiled=True)
    other_half = lax.ppermute(
        own_half, "grp", [(i, i ^ 1) for i in range(lax.axis_size("grp"))]
    )

    rows = pl.pallas_call(
        functools.partial(first_kernel, devices, groups),
        out_shape=pltpu.VMEM((clusters + channels * clusters + 1, 1, LANES), f32),
        in_specs=[SMEM] * 5 + [VMEM] * 3,
        out_specs=VMEM,
        scratch_shapes=[pltpu.VMEM((clusters, width // 8, 8, width), f32)] * BANKS,
        compiler_params=pltpu.CompilerParams(
            vmem_limit_bytes=16 << 20
        ),
        cost_estimate=pl.CostEstimate(flops=10**8, transcendentals=0, bytes_accessed=10**7),
        name="first",
    )(
        source_device,
        source_slot,
        receiver_slot,
        cluster_group,
        ambient,
        *in_vmem(own_half, form_factors, group_coupling),
    )
    share_rows = rows_for(channels, groups)
    new, share = pl.pallas_call(
        functools.partial(second_kernel, devices, groups, scale),
        out_shape=(own, pltpu.VMEM((devices * share_rows, 1, LANES), f32)),
        in_specs=[SMEM] * 4 + [VMEM] * 7,
        out_specs=(VMEM, VMEM),
        scratch_shapes=[pltpu.VMEM((clusters, 2, width // 8, 8, width), f32)] * BANKS,
        compiler_params=pltpu.CompilerParams(
            vmem_limit_bytes=16 << 20
        ),
        name="second",
    )(
        source_device,
        source_slot,
        receiver_slot,
        cluster_group,
        *in_vmem(
            own_half,
            other_half,
            form_factors,
            rows,
            by_channel(emission),
            by_channel(reflectance),
            patch_area,
        ),
    )
    shares = lax.all_to_all(share, AXES, split_axis=0, concat_axis=0, tiled=True)
    new, total = pl.pallas_call(
        functools.partial(total_kernel, devices, groups),
        out_shape=(
            pltpu.HBM((channels, clusters, width), f32),
            pltpu.HBM((channels, groups), f32),
        ),
        in_specs=[VMEM, VMEM],
        out_specs=(HBM, HBM),
        scratch_shapes=[pltpu.VMEM((channels, groups), f32), DMA((2,))],
        compiler_params=pltpu.CompilerParams(vmem_limit_bytes=4 << 20),
        name="total",
    )(*in_vmem(shares, new))
    return by_channel(new), total.T


def solution(mesh):
    split = AXES
    return jax.shard_map(
        on_device,
        mesh=mesh,
        in_specs=(
            P(split, None, None),
            P(split, None, None),
            P(split, None),
            P(split),
            P(split),
            P(split, None, None),
            P(split, None, None),
            P(split, None),
            P(split),
            P(),
            P(),
        ),
        out_specs=(P(split, None, None), P()),
        check_vma=False,
    )
```

```python
import functools

import jax
import jax.numpy as jnp
from jax import lax
from jax.experimental import pallas as pl
from jax.experimental.pallas import tpu as pltpu
from jax.sharding import PartitionSpec as P

LANES = 128
UNROLL = 16
BANKS = 2
PAD = 1
AXES = ("grp", "clu")
VMEM = pl.BlockSpec(memory_space=pltpu.VMEM)
SMEM = pl.BlockSpec(memory_space=pltpu.SMEM)
HBM = pl.BlockSpec(memory_space=pltpu.HBM)
DMA = pltpu.SemaphoreType.DMA


def in_hbm(*arrays):
    return tuple(pltpu.with_memory_space_constraint(a, pltpu.HBM) for a in arrays)


def in_vmem(*arrays):
    return tuple(pltpu.with_memory_space_constraint(a, pltpu.VMEM) for a in arrays)


def rows_for(quantities, groups):
    return -(-quantities // (LANES // groups))


def start_all(pairs, sems):
    copies = [pltpu.make_async_copy(src, dst, sems.at[i]) for i, (src, dst) in enumerate(pairs)]
    for copy in copies:
        copy.start()
    return copies


def pack_kernel(
    devices,
    pair_stride,
    groups,
    radiosity_hbm,
    area_hbm,
    cluster_group_hbm,
    source_device_hbm,
    source_slot_hbm,
    receiver_slot_hbm,
    ambient_hbm,
    out_ref,
    cluster_group_ref,
    source_device_ref,
    source_slot_ref,
    receiver_slot_ref,
    ambient_ref,
    radiosity_ref,
    area_ref,
    sems,
):
    channels, clusters, _ = radiosity_ref.shape
    per_row = LANES // groups
    copies = start_all(
        (
            (radiosity_hbm, radiosity_ref),
            (area_hbm, area_ref),
            (cluster_group_hbm, cluster_group_ref),
            (source_device_hbm, source_device_ref),
            (source_slot_hbm, source_slot_ref),
            (receiver_slot_hbm, receiver_slot_ref),
            (ambient_hbm, ambient_ref),
        ),
        sems,
    )
    for copy in copies[:3]:
        copy.wait()
    area = area_ref[...]
    sums = [
        jnp.sum(radiosity_ref[c] * area, axis=1, keepdims=True) for c in range(channels)
    ] + [jnp.sum(area, axis=1, keepdims=True)]
    lane = lax.broadcasted_iota(jnp.int32, (1, LANES), 1)
    info = [jnp.zeros((1, LANES), jnp.float32) for _ in range(rows_for(channels + 1, groups))]
    for q in range(channels + 1):
        for k in range(clusters):
            spot = (q % per_row) * groups + cluster_group_ref[k]
            info[q // per_row] += jnp.where(lane == spot, sums[q][k : k + 1], 0.0)
    half = clusters // 2
    halves = [
        [(0, k) for k in range(clusters)] + [(1, k) for k in range(half)],
        [(2, k) for k in range(clusters)] + [(1, k) for k in range(half, clusters)],
    ]
    block = len(halves[0]) + len(info)
    for d in range(devices):
        rows = [radiosity_ref[c, k : k + 1] for c, k in halves[d // pair_stride % 2]] + info
        for r, row in enumerate(rows):
            out_ref[d * block + r] = row
    for copy in copies[3:]:
        copy.wait()


def column_sums(acc, diagonal):
    column = jnp.sum(acc, axis=2, keepdims=True)
    spread = jnp.sum(jnp.where(diagonal, column, 0.0), axis=0)
    return jnp.sum(spread, axis=0, keepdims=True)


def diagonal_mask(width):
    shape = (width // 8, 8, width)
    patch = lax.broadcasted_iota(jnp.int32, shape, 0) * 8 + lax.broadcasted_iota(jnp.int32, shape, 1)
    return patch == lax.broadcasted_iota(jnp.int32, shape, 2)


def first_kernel(
    devices,
    groups,
    source_device_ref,
    source_slot_ref,
    receiver_slot_ref,
    cluster_group_ref,
    ambient_ref,
    own_ref,
    factors_ref,
    coupling_ref,
    rows_ref,
    *acc_refs,
):
    count, width, _ = factors_ref.shape
    clusters, blocks = acc_refs[0].shape[0], width // 8
    channels = ambient_ref.shape[0]
    half = clusters // 2
    block_rows = own_ref.shape[0] // devices
    own_rows = clusters + half
    per_row = LANES // groups

    for acc_ref in acc_refs:
        acc_ref[...] = jnp.zeros_like(acc_ref)

    def step(group, carried):
        for u in range(UNROLL):
            l = group * UNROLL + u
            k = receiver_slot_ref[l]
            place = source_device_ref[l] * block_rows + source_slot_ref[l]
            row = jnp.broadcast_to(own_ref[place], (8, width))
            acc_ref = acc_refs[u % len(acc_refs)]
            for b in range(blocks):
                acc_ref[k, b] += factors_ref[l, b * 8 : (b + 1) * 8, :] * row
        return carried

    lax.fori_loop(0, count // UNROLL, step, 0)

    totals = []
    for r in range(own_rows, block_rows):
        total = own_ref[r]
        for d in range(1, devices):
            total = total + own_ref[d * block_rows + r]
        totals.append(total)
    lane = lax.broadcasted_iota(jnp.int32, (1, LANES), 1)
    inside = lane < groups
    parts = []
    for q in range(channels + 1):
        row, shift = totals[q // per_row], (q % per_row) * groups
        part = pltpu.roll(row, LANES - shift, 1) if shift else row
        parts.append(jnp.where(inside, part, 0.0))
    group_area = jnp.where(inside, parts[channels], 1.0)
    all_area = jnp.sum(parts[channels], axis=1, keepdims=True)
    for c in range(channels):
        old_group = parts[c] / group_area
        root = ambient_ref[c] * (jnp.sum(parts[c], axis=1, keepdims=True) / all_area)
        for k in range(clusters):
            coupling = coupling_ref[pl.ds(cluster_group_ref[k], 1), :]
            coarse = (
                jnp.sum(coupling * old_group[:, :groups], axis=1, keepdims=True) / groups + root
            )
            rows_ref[clusters + c * clusters + k] = jnp.broadcast_to(coarse, (1, LANES))
    wide_area = group_area
    for q in range(1, per_row):
        wide_area = jnp.where(lane >= q * groups, pltpu.roll(group_area, q * groups, 1), wide_area)
    rows_ref[clusters + channels * clusters] = wide_area

    diagonal = diagonal_mask(width)
    for k in range(clusters):
        rows_ref[k] = column_sums(sum(acc_ref[k, :blocks] for acc_ref in acc_refs), diagonal)


def second_kernel(
    devices,
    groups,
    scale,
    source_device_ref,
    source_slot_ref,
    receiver_slot_ref,
    cluster_group_ref,
    own_ref,
    other_ref,
    factors_ref,
    rows_ref,
    emission_ref,
    reflectance_ref,
    area_ref,
    radiosity_ref,
    share_ref,
    *acc_refs,
):
    channels, clusters, width = emission_ref.shape
    count = factors_ref.shape[0]
    half = clusters // 2
    blocks = width // 8
    block_rows = own_ref.shape[0] // devices
    per_row = LANES // groups
    core = lax.rem(lax.axis_index("grp"), 2)

    for acc_ref in acc_refs:
        acc_ref[...] = jnp.zeros_like(acc_ref)

    def step(group, carried):
        for u in range(UNROLL):
            l = group * UNROLL + u
            k, slot = receiver_slot_ref[l], source_slot_ref[l]
            base = source_device_ref[l] * block_rows
            upper = (slot >= half).astype(jnp.int32)
            inner = base + slot - half * upper + clusters
            middle = jnp.where(
                upper == core,
                jnp.broadcast_to(own_ref[inner], (8, width)),
                jnp.broadcast_to(other_ref[inner], (8, width)),
            )
            rows = (middle, jnp.broadcast_to(other_ref[base + slot], (8, width)))
            acc_ref = acc_refs[u % len(acc_refs)]
            for b in range(blocks):
                f = factors_ref[l, b * 8 : (b + 1) * 8, :]
                for r in range(2):
                    acc_ref[k, r, b] += f * rows[r]
        return carried

    lax.fori_loop(0, count // UNROLL, step, 0)

    diagonal = diagonal_mask(width)
    lane = lax.broadcasted_iota(jnp.int32, (1, LANES), 1)
    shares = [jnp.zeros((1, LANES), jnp.float32) for _ in range(rows_for(channels, groups))]
    for k in range(clusters):
        mine = rows_ref[k]
        middle = column_sums(sum(acc_ref[k, 0, :blocks] for acc_ref in acc_refs), diagonal)
        others = column_sums(sum(acc_ref[k, 1, :blocks] for acc_ref in acc_refs), diagonal)
        by_channel = (
            jnp.where(core == 0, mine, others),
            middle,
            jnp.where(core == 0, others, mine),
        )
        for c in range(channels):
            coarse = rows_ref[clusters + c * clusters + k]
            new = emission_ref[c, k : k + 1] + reflectance_ref[c, k : k + 1] * (
                by_channel[c] * scale + coarse
            )
            radiosity_ref[c, k : k + 1] = new
            pulled = jnp.sum(new * area_ref[k : k + 1], axis=1, keepdims=True)
            spot = (c % per_row) * groups + cluster_group_ref[k]
            shares[c // per_row] += jnp.where(lane == spot, pulled, 0.0)
    for r in range(len(shares)):
        row = shares[r] / rows_ref[clusters + channels * clusters]
        for d in range(devices):
            share_ref[d * len(shares) + r] = row


def total_kernel(devices, groups, share_ref, new_ref, new_hbm, total_hbm, total_ref, sems):
    channels = new_ref.shape[0]
    per_row = LANES // groups
    count = share_ref.shape[0] // devices
    new_copy = pltpu.make_async_copy(new_ref, new_hbm, sems.at[0])
    new_copy.start()
    rows = []
    for r in range(count):
        total = share_ref[r]
        for d in range(1, devices):
            total = total + share_ref[d * count + r]
        rows.append(total)
    for c in range(channels):
        row, shift = rows[c // per_row], (c % per_row) * groups
        part = pltpu.roll(row, LANES - shift, 1) if shift else row
        total_ref[c : c + 1, :] = part[:, :groups]
    total_copy = pltpu.make_async_copy(total_ref, total_hbm, sems.at[1])
    total_copy.start()
    new_copy.wait()
    total_copy.wait()


def on_device(
    radiosity,
    form_factors,
    source_device,
    source_slot,
    receiver_slot,
    emission,
    reflectance,
    patch_area,
    cluster_group,
    group_coupling,
    ambient,
):
    clusters, channels, width = radiosity.shape
    count = form_factors.shape[0]
    groups = group_coupling.shape[0]
    devices = lax.axis_size("grp") * lax.axis_size("clu")
    scale = 2.0 * clusters / (width * count)
    pair_stride = lax.axis_size("clu")
    block = clusters + clusters // 2 + rows_for(channels + 1, groups)
    by_channel = functools.partial(jnp.transpose, axes=(1, 0, 2))
    f32, i32 = jnp.float32, jnp.int32
    own = pltpu.VMEM((channels, clusters, width), f32)

    packed, cluster_group, source_device, source_slot, receiver_slot, ambient = pl.pallas_call(
        functools.partial(pack_kernel, devices, pair_stride, groups),
        out_shape=(
            pltpu.VMEM((devices * block, 1, LANES), f32),
            pltpu.SMEM((clusters,), i32),
            pltpu.SMEM((count,), i32),
            pltpu.SMEM((count,), i32),
            pltpu.SMEM((count,), i32),
            pltpu.SMEM((channels,), f32),
        ),
        in_specs=[HBM] * 7,
        out_specs=(VMEM,) + (SMEM,) * 5,
        scratch_shapes=[
            pltpu.VMEM((channels, clusters, width), f32),
            pltpu.VMEM((clusters, width), f32),
            DMA((7,)),
        ],
        compiler_params=pltpu.CompilerParams(vmem_limit_bytes=4 << 20),
        cost_estimate=pl.CostEstimate(flops=10**10, transcendentals=0, bytes_accessed=10**8),
        name="pack",
    )(
        *in_hbm(
            by_channel(radiosity),
            patch_area,
            cluster_group,
            source_device[:, 0],
            source_slot,
            receiver_slot,
            ambient,
        )
    )
    own_half = lax.all_to_all(packed, AXES, split_axis=0, concat_axis=0, tiled=True)
    other_half = lax.ppermute(
        own_half, "grp", [(i, i ^ 1) for i in range(lax.axis_size("grp"))]
    )

    rows = pl.pallas_call(
        functools.partial(first_kernel, devices, groups),
        out_shape=pltpu.VMEM((clusters + channels * clusters + 1, 1, LANES), f32),
        in_specs=[SMEM] * 5 + [VMEM] * 3,
        out_specs=VMEM,
        scratch_shapes=[pltpu.VMEM((clusters, width // 8 + PAD, 8, width), f32)] * BANKS,
        compiler_params=pltpu.CompilerParams(vmem_limit_bytes=16 << 20),
        cost_estimate=pl.CostEstimate(flops=10**8, transcendentals=0, bytes_accessed=10**7),
        name="first",
    )(
        source_device,
        source_slot,
        receiver_slot,
        cluster_group,
        ambient,
        *in_vmem(own_half, form_factors, group_coupling),
    )
    share_rows = rows_for(channels, groups)
    new, share = pl.pallas_call(
        functools.partial(second_kernel, devices, groups, scale),
        out_shape=(own, pltpu.VMEM((devices * share_rows, 1, LANES), f32)),
        in_specs=[SMEM] * 4 + [VMEM] * 7,
        out_specs=(VMEM, VMEM),
        scratch_shapes=[pltpu.VMEM((clusters, 2, width // 8 + PAD, 8, width), f32)] * BANKS,
        compiler_params=pltpu.CompilerParams(vmem_limit_bytes=16 << 20),
        name="second",
    )(
        source_device,
        source_slot,
        receiver_slot,
        cluster_group,
        *in_vmem(
            own_half,
            other_half,
            form_factors,
            rows,
            by_channel(emission),
            by_channel(reflectance),
            patch_area,
        ),
    )
    shares = lax.all_to_all(share, AXES, split_axis=0, concat_axis=0, tiled=True)
    new, total = pl.pallas_call(
        functools.partial(total_kernel, devices, groups),
        out_shape=(
            pltpu.HBM((channels, clusters, width), f32),
            pltpu.HBM((channels, groups), f32),
        ),
        in_specs=[VMEM, VMEM],
        out_specs=(HBM, HBM),
        scratch_shapes=[pltpu.VMEM((channels, groups), f32), DMA((2,))],
        compiler_params=pltpu.CompilerParams(vmem_limit_bytes=4 << 20),
        name="total",
    )(*in_vmem(shares, new))
    return by_channel(new), total.T


def solution(mesh):
    split = AXES
    return jax.shard_map(
        on_device,
        mesh=mesh,
        in_specs=(
            P(split, None, None),
            P(split, None, None),
            P(split, None),
            P(split),
            P(split),
            P(split, None, None),
            P(split, None, None),
            P(split, None),
            P(split),
            P(),
            P(),
        ),
        out_specs=(P(split, None, None), P()),
        check_vma=False,
    )
```

```python
import functools

import jax
import jax.numpy as jnp
from jax import lax
from jax.experimental import pallas as pl
from jax.experimental.pallas import tpu as pltpu
from jax.sharding import PartitionSpec as P

LANES = 128
UNROLL = 16
BANKS = 2
PAD = 1
AXES = ("grp", "clu")
VMEM = pl.BlockSpec(memory_space=pltpu.VMEM)
SMEM = pl.BlockSpec(memory_space=pltpu.SMEM)
HBM = pl.BlockSpec(memory_space=pltpu.HBM)
DMA = pltpu.SemaphoreType.DMA


def in_hbm(*arrays):
    return tuple(pltpu.with_memory_space_constraint(a, pltpu.HBM) for a in arrays)


def in_vmem(*arrays):
    return tuple(pltpu.with_memory_space_constraint(a, pltpu.VMEM) for a in arrays)


def rows_for(quantities, groups):
    return -(-quantities // (LANES // groups))


def place(sums, cluster_group_ref, groups):
    clusters = sums[0].shape[0]
    per_row = LANES // groups
    lane = lax.broadcasted_iota(jnp.int32, (clusters, LANES), 1)
    cluster = lax.broadcasted_iota(jnp.int32, (clusters, LANES), 0)
    group = jnp.full((clusters, LANES), cluster_group_ref[0], jnp.int32)
    for k in range(1, clusters):
        group = jnp.where(cluster == k, cluster_group_ref[k], group)
    rows = []
    for first in range(0, len(sums), per_row):
        spread = jnp.zeros((clusters, LANES), jnp.float32)
        for q in range(first, min(first + per_row, len(sums))):
            spread = jnp.where(lane == (q - first) * groups + group, sums[q], spread)
        rows.append(jnp.sum(spread, axis=0, keepdims=True))
    return rows


def tree_sum(values):
    while len(values) > 1:
        values = [sum(values[i : i + 2]) for i in range(0, len(values), 2)]
    return values[0]


def start_all(pairs, sems):
    copies = [pltpu.make_async_copy(src, dst, sems.at[i]) for i, (src, dst) in enumerate(pairs)]
    for copy in copies:
        copy.start()
    return copies


def pack_kernel(
    devices,
    pair_stride,
    groups,
    radiosity_hbm,
    area_hbm,
    cluster_group_hbm,
    source_device_hbm,
    source_slot_hbm,
    receiver_slot_hbm,
    ambient_hbm,
    out_ref,
    cluster_group_ref,
    source_device_ref,
    source_slot_ref,
    receiver_slot_ref,
    ambient_ref,
    radiosity_ref,
    area_ref,
    sems,
):
    channels, clusters, _ = radiosity_ref.shape
    per_row = LANES // groups
    copies = start_all(
        (
            (radiosity_hbm, radiosity_ref),
            (area_hbm, area_ref),
            (cluster_group_hbm, cluster_group_ref),
            (source_device_hbm, source_device_ref),
            (source_slot_hbm, source_slot_ref),
            (receiver_slot_hbm, receiver_slot_ref),
            (ambient_hbm, ambient_ref),
        ),
        sems,
    )
    for copy in copies[:3]:
        copy.wait()
    area = area_ref[...]
    sums = [
        jnp.sum(radiosity_ref[c] * area, axis=1, keepdims=True) for c in range(channels)
    ] + [jnp.sum(area, axis=1, keepdims=True)]
    info = place(sums, cluster_group_ref, groups)
    half = clusters // 2
    halves = [
        [(0, k) for k in range(clusters)] + [(1, k) for k in range(half)],
        [(2, k) for k in range(clusters)] + [(1, k) for k in range(half, clusters)],
    ]
    block = len(halves[0]) + len(info)
    for d in range(devices):
        rows = [radiosity_ref[c, k : k + 1] for c, k in halves[d // pair_stride % 2]] + info
        for r, row in enumerate(rows):
            out_ref[d * block + r] = row
    for copy in copies[3:]:
        copy.wait()


def column_sums(acc, diagonal):
    column = jnp.sum(acc, axis=2, keepdims=True)
    spread = jnp.sum(jnp.where(diagonal, column, 0.0), axis=0)
    return jnp.sum(spread, axis=0, keepdims=True)


def diagonal_mask(width):
    shape = (width // 8, 8, width)
    patch = lax.broadcasted_iota(jnp.int32, shape, 0) * 8 + lax.broadcasted_iota(jnp.int32, shape, 1)
    return patch == lax.broadcasted_iota(jnp.int32, shape, 2)


def first_kernel(
    devices,
    groups,
    source_device_ref,
    source_slot_ref,
    receiver_slot_ref,
    cluster_group_ref,
    ambient_ref,
    own_ref,
    factors_ref,
    coupling_ref,
    rows_ref,
    *acc_refs,
):
    count, width, _ = factors_ref.shape
    clusters, blocks = acc_refs[0].shape[0], width // 8
    channels = ambient_ref.shape[0]
    half = clusters // 2
    block_rows = own_ref.shape[0] // devices
    own_rows = clusters + half
    per_row = LANES // groups

    for acc_ref in acc_refs:
        acc_ref[...] = jnp.zeros_like(acc_ref)

    def step(group, carried):
        for u in range(UNROLL):
            l = group * UNROLL + u
            k = receiver_slot_ref[l]
            place = source_device_ref[l] * block_rows + source_slot_ref[l]
            row = jnp.broadcast_to(own_ref[place], (8, width))
            acc_ref = acc_refs[u % len(acc_refs)]
            for b in range(blocks):
                acc_ref[k, b] += factors_ref[l, b * 8 : (b + 1) * 8, :] * row
        return carried

    totals = [
        tree_sum([own_ref[d * block_rows + r] for d in range(devices)])
        for r in range(own_rows, block_rows)
    ]
    lane = lax.broadcasted_iota(jnp.int32, (1, LANES), 1)
    inside = lane < groups
    parts = []
    for q in range(channels + 1):
        row, shift = totals[q // per_row], (q % per_row) * groups
        part = pltpu.roll(row, LANES - shift, 1) if shift else row
        parts.append(jnp.where(inside, part, 0.0))
    group_area = jnp.where(inside, parts[channels], 1.0)
    all_area = jnp.sum(parts[channels], axis=1, keepdims=True)
    for c in range(channels):
        old_group = parts[c] / group_area
        root = ambient_ref[c] * (jnp.sum(parts[c], axis=1, keepdims=True) / all_area)
        for k in range(clusters):
            coupling = coupling_ref[pl.ds(cluster_group_ref[k], 1), :]
            coarse = (
                jnp.sum(coupling * old_group[:, :groups], axis=1, keepdims=True) / groups + root
            )
            rows_ref[clusters + c * clusters + k] = jnp.broadcast_to(coarse, (1, LANES))
    wide_area = group_area
    for q in range(1, per_row):
        wide_area = jnp.where(lane >= q * groups, pltpu.roll(group_area, q * groups, 1), wide_area)
    rows_ref[clusters + channels * clusters] = 1.0 / wide_area

    step(0, 0)
    lax.fori_loop(1, count // UNROLL, step, 0)

    diagonal = diagonal_mask(width)
    for k in range(clusters):
        rows_ref[k] = column_sums(sum(acc_ref[k, :blocks] for acc_ref in acc_refs), diagonal)


def second_kernel(
    devices,
    groups,
    scale,
    source_device_ref,
    source_slot_ref,
    receiver_slot_ref,
    cluster_group_ref,
    own_ref,
    other_ref,
    factors_ref,
    rows_ref,
    emission_ref,
    reflectance_ref,
    area_ref,
    radiosity_ref,
    share_ref,
    *acc_refs,
):
    channels, clusters, width = emission_ref.shape
    count = factors_ref.shape[0]
    half = clusters // 2
    blocks = width // 8
    block_rows = own_ref.shape[0] // devices
    per_row = LANES // groups
    core = lax.rem(lax.axis_index("grp"), 2)

    for acc_ref in acc_refs:
        acc_ref[...] = jnp.zeros_like(acc_ref)

    def step(group, carried):
        for u in range(UNROLL):
            l = group * UNROLL + u
            k, slot = receiver_slot_ref[l], source_slot_ref[l]
            base = source_device_ref[l] * block_rows
            upper = (slot >= half).astype(jnp.int32)
            inner = base + slot - half * upper + clusters
            middle = jnp.where(
                upper == core,
                jnp.broadcast_to(own_ref[inner], (8, width)),
                jnp.broadcast_to(other_ref[inner], (8, width)),
            )
            rows = (middle, jnp.broadcast_to(other_ref[base + slot], (8, width)))
            acc_ref = acc_refs[u % len(acc_refs)]
            for b in range(blocks):
                f = factors_ref[l, b * 8 : (b + 1) * 8, :]
                for r in range(2):
                    acc_ref[k, r, b] += f * rows[r]
        return carried

    lax.fori_loop(0, count // UNROLL, step, 0)

    diagonal = diagonal_mask(width)
    for k in range(clusters):
        mine = rows_ref[k]
        middle = column_sums(sum(acc_ref[k, 0, :blocks] for acc_ref in acc_refs), diagonal)
        others = column_sums(sum(acc_ref[k, 1, :blocks] for acc_ref in acc_refs), diagonal)
        by_channel = (
            jnp.where(core == 0, mine, others),
            middle,
            jnp.where(core == 0, others, mine),
        )
        for c in range(channels):
            coarse = rows_ref[clusters + c * clusters + k]
            radiosity_ref[c, k : k + 1] = emission_ref[c, k : k + 1] + reflectance_ref[
                c, k : k + 1
            ] * (by_channel[c] * scale + coarse)
    pulled = [
        jnp.sum(radiosity_ref[c] * area_ref[...], axis=1, keepdims=True) for c in range(channels)
    ]
    shares = place(pulled, cluster_group_ref, groups)
    for r in range(len(shares)):
        row = shares[r] * rows_ref[clusters + channels * clusters]
        for d in range(devices):
            share_ref[d * len(shares) + r] = row


def total_kernel(devices, groups, share_ref, new_ref, new_hbm, total_hbm, total_ref, sems):
    channels = new_ref.shape[0]
    per_row = LANES // groups
    count = share_ref.shape[0] // devices
    new_copy = pltpu.make_async_copy(new_ref, new_hbm, sems.at[0])
    new_copy.start()
    rows = [tree_sum([share_ref[d * count + r] for d in range(devices)]) for r in range(count)]
    for c in range(channels):
        row, shift = rows[c // per_row], (c % per_row) * groups
        part = pltpu.roll(row, LANES - shift, 1) if shift else row
        total_ref[c : c + 1, :] = part[:, :groups]
    total_copy = pltpu.make_async_copy(total_ref, total_hbm, sems.at[1])
    total_copy.start()
    new_copy.wait()
    total_copy.wait()


def on_device(
    radiosity,
    form_factors,
    source_device,
    source_slot,
    receiver_slot,
    emission,
    reflectance,
    patch_area,
    cluster_group,
    group_coupling,
    ambient,
):
    clusters, channels, width = radiosity.shape
    count = form_factors.shape[0]
    groups = group_coupling.shape[0]
    devices = lax.axis_size("grp") * lax.axis_size("clu")
    scale = 2.0 * clusters / (width * count)
    pair_stride = lax.axis_size("clu")
    block = clusters + clusters // 2 + rows_for(channels + 1, groups)
    by_channel = functools.partial(jnp.transpose, axes=(1, 0, 2))
    f32, i32 = jnp.float32, jnp.int32
    own = pltpu.VMEM((channels, clusters, width), f32)

    packed, cluster_group, source_device, source_slot, receiver_slot, ambient = pl.pallas_call(
        functools.partial(pack_kernel, devices, pair_stride, groups),
        out_shape=(
            pltpu.VMEM((devices * block, 1, LANES), f32),
            pltpu.SMEM((clusters,), i32),
            pltpu.SMEM((count,), i32),
            pltpu.SMEM((count,), i32),
            pltpu.SMEM((count,), i32),
            pltpu.SMEM((channels,), f32),
        ),
        in_specs=[HBM] * 7,
        out_specs=(VMEM,) + (SMEM,) * 5,
        scratch_shapes=[
            pltpu.VMEM((channels, clusters, width), f32),
            pltpu.VMEM((clusters, width), f32),
            DMA((7,)),
        ],
        compiler_params=pltpu.CompilerParams(vmem_limit_bytes=4 << 20),
        cost_estimate=pl.CostEstimate(flops=10**10, transcendentals=0, bytes_accessed=10**8),
        name="pack",
    )(
        *in_hbm(
            by_channel(radiosity),
            patch_area,
            cluster_group,
            source_device[:, 0],
            source_slot,
            receiver_slot,
            ambient,
        )
    )
    own_half = lax.all_to_all(packed, AXES, split_axis=0, concat_axis=0, tiled=True)
    other_half = lax.ppermute(
        own_half, "grp", [(i, i ^ 1) for i in range(lax.axis_size("grp"))]
    )

    rows = pl.pallas_call(
        functools.partial(first_kernel, devices, groups),
        out_shape=pltpu.VMEM((clusters + channels * clusters + 1, 1, LANES), f32),
        in_specs=[SMEM] * 5 + [VMEM] * 3,
        out_specs=VMEM,
        scratch_shapes=[pltpu.VMEM((clusters, width // 8 + PAD, 8, width), f32)] * BANKS,
        compiler_params=pltpu.CompilerParams(vmem_limit_bytes=16 << 20),
        cost_estimate=pl.CostEstimate(flops=10**8, transcendentals=0, bytes_accessed=10**7),
        name="first",
    )(
        source_device,
        source_slot,
        receiver_slot,
        cluster_group,
        ambient,
        *in_vmem(own_half, form_factors, group_coupling),
    )
    share_rows = rows_for(channels, groups)
    new, share = pl.pallas_call(
        functools.partial(second_kernel, devices, groups, scale),
        out_shape=(own, pltpu.VMEM((devices * share_rows, 1, LANES), f32)),
        in_specs=[SMEM] * 4 + [VMEM] * 7,
        out_specs=(VMEM, VMEM),
        scratch_shapes=[pltpu.VMEM((clusters, 2, width // 8 + PAD, 8, width), f32)] * BANKS,
        compiler_params=pltpu.CompilerParams(vmem_limit_bytes=16 << 20),
        name="second",
    )(
        source_device,
        source_slot,
        receiver_slot,
        cluster_group,
        *in_vmem(
            own_half,
            other_half,
            form_factors,
            rows,
            by_channel(emission),
            by_channel(reflectance),
            patch_area,
        ),
    )
    shares = lax.all_to_all(share, AXES, split_axis=0, concat_axis=0, tiled=True)
    new, total = pl.pallas_call(
        functools.partial(total_kernel, devices, groups),
        out_shape=(
            pltpu.HBM((channels, clusters, width), f32),
            pltpu.HBM((channels, groups), f32),
        ),
        in_specs=[VMEM, VMEM],
        out_specs=(HBM, HBM),
        scratch_shapes=[pltpu.VMEM((channels, groups), f32), DMA((2,))],
        compiler_params=pltpu.CompilerParams(vmem_limit_bytes=4 << 20),
        name="total",
    )(*in_vmem(shares, new))
    return by_channel(new), total.T


def solution(mesh):
    split = AXES
    return jax.shard_map(
        on_device,
        mesh=mesh,
        in_specs=(
            P(split, None, None),
            P(split, None, None),
            P(split, None),
            P(split),
            P(split),
            P(split, None, None),
            P(split, None, None),
            P(split, None),
            P(split),
            P(),
            P(),
        ),
        out_specs=(P(split, None, None), P()),
        check_vma=False,
    )
```

```python
import functools

import jax
import jax.numpy as jnp
from jax import lax
from jax.experimental import pallas as pl
from jax.experimental.pallas import tpu as pltpu
from jax.sharding import PartitionSpec as P

LANES = 128
UNROLL = 16
BANKS = 2
PAD = 1
AXES = ("grp", "clu")
VMEM = pl.BlockSpec(memory_space=pltpu.VMEM)
SMEM = pl.BlockSpec(memory_space=pltpu.SMEM)
HBM = pl.BlockSpec(memory_space=pltpu.HBM)
DMA = pltpu.SemaphoreType.DMA


def in_hbm(*arrays):
    return tuple(pltpu.with_memory_space_constraint(a, pltpu.HBM) for a in arrays)


def in_vmem(*arrays):
    return tuple(pltpu.with_memory_space_constraint(a, pltpu.VMEM) for a in arrays)


def rows_for(quantities, groups):
    return -(-quantities // (LANES // groups))


def place(sums, cluster_group_ref, groups):
    clusters = sums[0].shape[0]
    per_row = LANES // groups
    lane = lax.broadcasted_iota(jnp.int32, (clusters, LANES), 1)
    cluster = lax.broadcasted_iota(jnp.int32, (clusters, LANES), 0)
    group = jnp.full((clusters, LANES), cluster_group_ref[0], jnp.int32)
    for k in range(1, clusters):
        group = jnp.where(cluster == k, cluster_group_ref[k], group)
    rows = []
    for first in range(0, len(sums), per_row):
        spread = jnp.zeros((clusters, LANES), jnp.float32)
        for q in range(first, min(first + per_row, len(sums))):
            spread = jnp.where(lane == (q - first) * groups + group, sums[q], spread)
        rows.append(jnp.sum(spread, axis=0, keepdims=True))
    return rows


def tree_sum(values):
    while len(values) > 1:
        values = [sum(values[i : i + 2]) for i in range(0, len(values), 2)]
    return values[0]


def start_all(pairs, sems):
    copies = [pltpu.make_async_copy(src, dst, sems.at[i]) for i, (src, dst) in enumerate(pairs)]
    for copy in copies:
        copy.start()
    return copies


def pack_kernel(
    devices,
    pair_stride,
    groups,
    radiosity_hbm,
    area_hbm,
    cluster_group_hbm,
    source_device_hbm,
    source_slot_hbm,
    receiver_slot_hbm,
    ambient_hbm,
    out_ref,
    cluster_group_ref,
    index_ref,
    ambient_ref,
    radiosity_ref,
    area_ref,
    sems,
):
    channels, clusters, _ = radiosity_ref.shape
    per_row = LANES // groups
    copies = start_all(
        (
            (radiosity_hbm, radiosity_ref),
            (area_hbm, area_ref),
            (cluster_group_hbm, cluster_group_ref),
            (ambient_hbm, ambient_ref),
        ),
        sems,
    )
    count = source_slot_hbm.shape[0]
    for i, array in enumerate((source_device_hbm, source_slot_hbm, receiver_slot_hbm)):
        pltpu.make_async_copy(array, index_ref.at[pl.ds(i * count, count)], sems.at[4]).start()
    for copy in copies[:3]:
        copy.wait()
    area = area_ref[...]
    sums = [
        jnp.sum(radiosity_ref[c] * area, axis=1, keepdims=True) for c in range(channels)
    ] + [jnp.sum(area, axis=1, keepdims=True)]
    info = place(sums, cluster_group_ref, groups)
    half = clusters // 2
    halves = [
        [(0, k) for k in range(clusters)] + [(1, k) for k in range(half)],
        [(2, k) for k in range(clusters)] + [(1, k) for k in range(half, clusters)],
    ]
    block = len(halves[0]) + len(info)
    for d in range(devices):
        rows = [radiosity_ref[c, k : k + 1] for c, k in halves[d // pair_stride % 2]] + info
        for r, row in enumerate(rows):
            out_ref[d * block + r] = row
    copies[3].wait()
    pltpu.make_async_copy(index_ref, index_ref, sems.at[4]).wait()


def column_sums(acc, diagonal):
    column = jnp.sum(acc, axis=2, keepdims=True)
    spread = jnp.sum(jnp.where(diagonal, column, 0.0), axis=0)
    return jnp.sum(spread, axis=0, keepdims=True)


def diagonal_mask(width):
    shape = (width // 8, 8, width)
    patch = lax.broadcasted_iota(jnp.int32, shape, 0) * 8 + lax.broadcasted_iota(jnp.int32, shape, 1)
    return patch == lax.broadcasted_iota(jnp.int32, shape, 2)


def first_kernel(
    devices,
    groups,
    index_ref,
    cluster_group_ref,
    ambient_ref,
    own_ref,
    factors_ref,
    coupling_ref,
    rows_ref,
    *acc_refs,
):
    count, width, _ = factors_ref.shape
    clusters, blocks = acc_refs[0].shape[0], width // 8
    channels = ambient_ref.shape[0]
    half = clusters // 2
    block_rows = own_ref.shape[0] // devices
    own_rows = clusters + half
    per_row = LANES // groups

    for acc_ref in acc_refs:
        acc_ref[...] = jnp.zeros_like(acc_ref)

    def step(group, carried):
        for u in range(UNROLL):
            l = group * UNROLL + u
            k = index_ref[2 * count + l]
            place = index_ref[l] * block_rows + index_ref[count + l]
            row = jnp.broadcast_to(own_ref[place], (8, width))
            acc_ref = acc_refs[u % len(acc_refs)]
            for b in range(blocks):
                acc_ref[k, b] += factors_ref[l, b * 8 : (b + 1) * 8, :] * row
        return carried

    totals = [
        tree_sum([own_ref[d * block_rows + r] for d in range(devices)])
        for r in range(own_rows, block_rows)
    ]
    lane = lax.broadcasted_iota(jnp.int32, (1, LANES), 1)
    inside = lane < groups
    parts = []
    for q in range(channels + 1):
        row, shift = totals[q // per_row], (q % per_row) * groups
        part = pltpu.roll(row, LANES - shift, 1) if shift else row
        parts.append(jnp.where(inside, part, 0.0))
    group_area = jnp.where(inside, parts[channels], 1.0)
    all_area = jnp.sum(parts[channels], axis=1, keepdims=True)
    for c in range(channels):
        old_group = parts[c] / group_area
        root = ambient_ref[c] * (jnp.sum(parts[c], axis=1, keepdims=True) / all_area)
        for k in range(clusters):
            coupling = coupling_ref[pl.ds(cluster_group_ref[k], 1), :]
            coarse = (
                jnp.sum(coupling * old_group[:, :groups], axis=1, keepdims=True) / groups + root
            )
            rows_ref[clusters + c * clusters + k] = jnp.broadcast_to(coarse, (1, LANES))
    wide_area = group_area
    for q in range(1, per_row):
        wide_area = jnp.where(lane >= q * groups, pltpu.roll(group_area, q * groups, 1), wide_area)
    rows_ref[clusters + channels * clusters] = 1.0 / wide_area

    step(0, 0)
    lax.fori_loop(1, count // UNROLL, step, 0)

    diagonal = diagonal_mask(width)
    for k in range(clusters):
        rows_ref[k] = column_sums(sum(acc_ref[k, :blocks] for acc_ref in acc_refs), diagonal)


def second_kernel(
    devices,
    groups,
    scale,
    index_ref,
    cluster_group_ref,
    own_ref,
    other_ref,
    factors_ref,
    rows_ref,
    emission_ref,
    reflectance_ref,
    area_ref,
    radiosity_ref,
    share_ref,
    *acc_refs,
):
    channels, clusters, width = emission_ref.shape
    count = factors_ref.shape[0]
    half = clusters // 2
    blocks = width // 8
    block_rows = own_ref.shape[0] // devices
    per_row = LANES // groups
    core = lax.rem(lax.axis_index("grp"), 2)

    for acc_ref in acc_refs:
        acc_ref[...] = jnp.zeros_like(acc_ref)

    def step(group, carried):
        for u in range(UNROLL):
            l = group * UNROLL + u
            k, slot = index_ref[2 * count + l], index_ref[count + l]
            base = index_ref[l] * block_rows
            upper = (slot >= half).astype(jnp.int32)
            inner = base + slot - half * upper + clusters
            middle = jnp.where(
                upper == core,
                jnp.broadcast_to(own_ref[inner], (8, width)),
                jnp.broadcast_to(other_ref[inner], (8, width)),
            )
            rows = (middle, jnp.broadcast_to(other_ref[base + slot], (8, width)))
            acc_ref = acc_refs[u % len(acc_refs)]
            for b in range(blocks):
                f = factors_ref[l, b * 8 : (b + 1) * 8, :]
                for r in range(2):
                    acc_ref[k, r, b] += f * rows[r]
        return carried

    lax.fori_loop(0, count // UNROLL, step, 0)

    diagonal = diagonal_mask(width)
    for k in range(clusters):
        mine = rows_ref[k]
        middle = column_sums(sum(acc_ref[k, 0, :blocks] for acc_ref in acc_refs), diagonal)
        others = column_sums(sum(acc_ref[k, 1, :blocks] for acc_ref in acc_refs), diagonal)
        by_channel = (
            jnp.where(core == 0, mine, others),
            middle,
            jnp.where(core == 0, others, mine),
        )
        for c in range(channels):
            coarse = rows_ref[clusters + c * clusters + k]
            radiosity_ref[c, k : k + 1] = emission_ref[c, k : k + 1] + reflectance_ref[
                c, k : k + 1
            ] * (by_channel[c] * scale + coarse)
    pulled = [
        jnp.sum(radiosity_ref[c] * area_ref[...], axis=1, keepdims=True) for c in range(channels)
    ]
    shares = place(pulled, cluster_group_ref, groups)
    for r in range(len(shares)):
        row = shares[r] * rows_ref[clusters + channels * clusters]
        for d in range(devices):
            share_ref[d * len(shares) + r] = row


def total_kernel(devices, groups, share_ref, new_ref, new_hbm, total_hbm, total_ref, sems):
    channels = new_ref.shape[0]
    per_row = LANES // groups
    count = share_ref.shape[0] // devices
    new_copy = pltpu.make_async_copy(new_ref, new_hbm, sems.at[0])
    new_copy.start()
    rows = [tree_sum([share_ref[d * count + r] for d in range(devices)]) for r in range(count)]
    for c in range(channels):
        row, shift = rows[c // per_row], (c % per_row) * groups
        part = pltpu.roll(row, LANES - shift, 1) if shift else row
        total_ref[c : c + 1, :] = part[:, :groups]
    total_copy = pltpu.make_async_copy(total_ref, total_hbm, sems.at[1])
    total_copy.start()
    new_copy.wait()
    total_copy.wait()


def on_device(
    radiosity,
    form_factors,
    source_device,
    source_slot,
    receiver_slot,
    emission,
    reflectance,
    patch_area,
    cluster_group,
    group_coupling,
    ambient,
):
    clusters, channels, width = radiosity.shape
    count = form_factors.shape[0]
    groups = group_coupling.shape[0]
    devices = lax.axis_size("grp") * lax.axis_size("clu")
    scale = 2.0 * clusters / (width * count)
    pair_stride = lax.axis_size("clu")
    block = clusters + clusters // 2 + rows_for(channels + 1, groups)
    by_channel = functools.partial(jnp.transpose, axes=(1, 0, 2))
    f32, i32 = jnp.float32, jnp.int32
    own = pltpu.VMEM((channels, clusters, width), f32)

    packed, cluster_group, index, ambient = pl.pallas_call(
        functools.partial(pack_kernel, devices, pair_stride, groups),
        out_shape=(
            pltpu.VMEM((devices * block, 1, LANES), f32),
            pltpu.SMEM((clusters,), i32),
            pltpu.SMEM((3 * count,), i32),
            pltpu.SMEM((channels,), f32),
        ),
        in_specs=[HBM] * 7,
        out_specs=(VMEM,) + (SMEM,) * 3,
        scratch_shapes=[
            pltpu.VMEM((channels, clusters, width), f32),
            pltpu.VMEM((clusters, width), f32),
            DMA((5,)),
        ],
        compiler_params=pltpu.CompilerParams(vmem_limit_bytes=4 << 20),
        cost_estimate=pl.CostEstimate(flops=10**10, transcendentals=0, bytes_accessed=10**8),
        name="pack",
    )(
        *in_hbm(
            by_channel(radiosity),
            patch_area,
            cluster_group,
            source_device[:, 0],
            source_slot,
            receiver_slot,
            ambient,
        )
    )
    own_half = lax.all_to_all(packed, AXES, split_axis=0, concat_axis=0, tiled=True)
    other_half = lax.ppermute(
        own_half, "grp", [(i, i ^ 1) for i in range(lax.axis_size("grp"))]
    )

    rows = pl.pallas_call(
        functools.partial(first_kernel, devices, groups),
        out_shape=pltpu.VMEM((clusters + channels * clusters + 1, 1, LANES), f32),
        in_specs=[SMEM] * 3 + [VMEM] * 3,
        out_specs=VMEM,
        scratch_shapes=[pltpu.VMEM((clusters, width // 8 + 2 * PAD, 8, width), f32)] * BANKS,
        compiler_params=pltpu.CompilerParams(vmem_limit_bytes=16 << 20),
        cost_estimate=pl.CostEstimate(flops=10**8, transcendentals=0, bytes_accessed=10**7),
        name="first",
    )(
        index,
        cluster_group,
        ambient,
        *in_vmem(own_half, form_factors, group_coupling),
    )
    share_rows = rows_for(channels, groups)
    new, share = pl.pallas_call(
        functools.partial(second_kernel, devices, groups, scale),
        out_shape=(own, pltpu.VMEM((devices * share_rows, 1, LANES), f32)),
        in_specs=[SMEM] * 2 + [VMEM] * 7,
        out_specs=(VMEM, VMEM),
        scratch_shapes=[pltpu.VMEM((clusters, 2, width // 8 + PAD, 8, width), f32)] * BANKS,
        compiler_params=pltpu.CompilerParams(vmem_limit_bytes=16 << 20),
        name="second",
    )(
        index,
        cluster_group,
        *in_vmem(
            own_half,
            other_half,
            form_factors,
            rows,
            by_channel(emission),
            by_channel(reflectance),
            patch_area,
        ),
    )
    shares = lax.all_to_all(share, AXES, split_axis=0, concat_axis=0, tiled=True)
    new, total = pl.pallas_call(
        functools.partial(total_kernel, devices, groups),
        out_shape=(
            pltpu.HBM((channels, clusters, width), f32),
            pltpu.HBM((channels, groups), f32),
        ),
        in_specs=[VMEM, VMEM],
        out_specs=(HBM, HBM),
        scratch_shapes=[pltpu.VMEM((channels, groups), f32), DMA((2,))],
        compiler_params=pltpu.CompilerParams(vmem_limit_bytes=4 << 20),
        name="total",
    )(*in_vmem(shares, new))
    return by_channel(new), total.T


def solution(mesh):
    split = AXES
    return jax.shard_map(
        on_device,
        mesh=mesh,
        in_specs=(
            P(split, None, None),
            P(split, None, None),
            P(split, None),
            P(split),
            P(split),
            P(split, None, None),
            P(split, None, None),
            P(split, None),
            P(split),
            P(),
            P(),
        ),
        out_specs=(P(split, None, None), P()),
        check_vma=False,
    )
```
